512 devices in a mesh: gx: 8 (over z), gy: 4 (over x), gz: 16 (over y, core).
Axes of the slice: x: 4, y: 8, z: 8, core: 2. Of those that a mesh axis runs over, the one named last changes fastest.
Arguments:
- velocity: float32 [3, 64, 32, 2048], P(None, 'gx', 'gy', 'gz'), may hold values from -6 to 6
- direction: float32 [3, 64, 32, 2048], P(None, 'gx', 'gy', 'gz'), may hold values from -3 to 3
- pressure: float32 [64, 32, 2048], P('gx', 'gy', 'gz'), may hold values from -6 to 6
- body_force: float32 [3, 64, 32, 2048], P(None, 'gx', 'gy', 'gz'), may hold values from -21 to 21, as said below
- phase_ids: int32 [64, 32, 2048], P('gx', 'gy', 'gz'), may hold values from 0 to 3
- creep_factor: float32 [4], replicated, may hold values from 0.5 to 2
- stress_exponent: float32 [4], replicated, may hold values from 1.5 to 4
- yield_stress: float32 [4], replicated, may hold values from 0.5 to 3
- accepted: int32 [1], replicated, may hold values from 0 to 3
Outputs:
- norms: float32 [2, 4], replicated
- chosen_velocity: float32 [3, 64, 32, 2048], P(None, 'gx', 'gy', 'gz')
- chosen_residual: float32 [3, 64, 32, 2048], P(None, 'gx', 'gy', 'gz')
The draws below stay inside these ranges and needn't reach their ends.
Inputs may be any that keep to these rules, and one draw needn't show every extreme that they name: `body_force`: body force on every cell and component.
All inputs are finite; a program needn't handle non-finite values.
Results may differ from the reference program's by a relative error of at most 0.00022.
Values sent between devices are 32-bit elements; how exact they have to be, the bound alone decides.
A program may use at most 64 MiB of HBM per device.

```python
import math
import jax
import jax.numpy as jnp
from jax import lax

NPHASE = 4
NX = 64
NY = 32
NZ = 2048


def draw_body_force(key, part):
    xpos = jnp.arange(NX, dtype=jnp.float32) / NX
    ypos = jnp.arange(NY, dtype=jnp.float32) / NY
    zpos = jnp.arange(NZ, dtype=jnp.float32) / NZ
    growth = jnp.power(3.0, 0.5 * (xpos[:, None, None] + ypos[None, :, None] + zpos[None, None, :]))
    rough = jax.random.truncated_normal(jax.random.fold_in(key, 7), -4.0, 4.0, (3, NX, NY, NZ), jnp.float32)
    return rough * growth[None]


def place_ends(result, stream_key, smallest, top_value):
    longest = result.shape.index(max(result.shape))
    spots = []
    for shift in (0, 1):
        where = [jax.random.randint(jax.random.fold_in(stream_key, axis), (), 0, length) for axis, length in enumerate(result.shape)]
        where[longest] = (where[longest] + shift) % result.shape[longest]
        spots.append(tuple(where))
    return result.at[spots[0]].set(smallest).at[spots[1]].set(top_value)


def steps_of(rng, shape, shards, smallest, largest):
    factor_of = 1.0
    for axis_at, shards_of in shards:
        draws = jax.random.uniform(jax.random.fold_in(jax.random.fold_in(rng, 6), axis_at), (shards_of,), jnp.float32, smallest / len(shards), largest / len(shards))
        factor_of = factor_of * jnp.repeat(jnp.exp(draws), shape[axis_at] // shards_of).reshape((-1,) + (1,) * (len(shape) - 1 - axis_at))
    return factor_of


def bell_draw(own_key, extent, deviation, most, split=(), held_as=jnp.bfloat16):
    result = jax.random.normal(own_key, extent, jnp.float32) * deviation
    if len(split) > 0:
        result = steps_of(own_key, extent, split, -0.22, 0.18) * result
    return jnp.clip(result, min=-most, max=most).astype(held_as)


def setup_inputs(seed: int = 0) -> dict:
    key_of = jax.random.split(jax.random.key(seed), 10)
    velocity = bell_draw(key_of[0], (3, NX, NY, NZ), 1.0, 6.0, ((1, 8), (2, 4), (3, 16)), jnp.float32)
    direction = bell_draw(key_of[1], (3, NX, NY, NZ), 0.5, 3.0, ((1, 8), (2, 4), (3, 16)), jnp.float32)
    pressure = bell_draw(key_of[2], (NX, NY, NZ), 1.0, 6.0, ((0, 8), (1, 4), (2, 16)), jnp.float32)
    body_force = draw_body_force(jax.random.fold_in(key_of[9], 71), 0)
    phase_ids = place_ends(jax.random.randint(key_of[4], (NX, NY, NZ), 0, NPHASE), jax.random.fold_in(key_of[4], 1), 0, NPHASE - 1).astype(jnp.int32)
    creep_factor = jnp.clip(jnp.exp(jax.random.uniform(key_of[5], (NPHASE,), jnp.float32, math.log(0.5), math.log(2.0))), 0.5, 2.0)
    stress_exponent = jnp.clip(jax.random.uniform(key_of[6], (NPHASE,), jnp.float32, 1.5, 4.0), 1.5, 4.0)
    yield_stress = jnp.clip(jnp.exp(jax.random.uniform(key_of[7], (NPHASE,), jnp.float32, math.log(0.5), math.log(3.0))), 0.5, 3.0)
    accepted = jax.random.randint(key_of[8], (1,), 0, 4).astype(jnp.int32)
    return dict(velocity=velocity, direction=direction, pressure=pressure, body_force=body_force, phase_ids=phase_ids, creep_factor=creep_factor, stress_exponent=stress_exponent, yield_stress=yield_stress, accepted=accepted)


step_lengths = (1.0, 0.5, 0.25, 0.125)
rate_offset = 0.01
viscosity_least = 0.05
tiny_mean = 1e-06
tensor_slots = ((0, 3, 4), (3, 1, 5), (4, 5, 2))

def centered(values, axis_number):
    lower = [slice(1, -1)] * 3
    upper = [slice(1, -1)] * 3
    lower[axis_number] = slice(0, -2)
    upper[axis_number] = slice(2, None)
    leading = (slice(None),) * (values.ndim - 3)
    return 0.5 * (values[leading + tuple(upper)] - values[leading + tuple(lower)])

def component(values, i):
    return lax.index_in_dim(values, i, values.ndim - 4, keepdims=False)

def strain_rates(padded):
    gradients = [[centered(component(padded, i), j) for j in range(3)] for i in range(3)]
    return jnp.stack([gradients[0][0], gradients[1][1], gradients[2][2], 0.5 * (gradients[0][1] + gradients[1][0]), 0.5 * (gradients[0][2] + gradients[2][0]), 0.5 * (gradients[1][2] + gradients[2][1])], axis=-4)

def double_dot(first, second):
    diagonal = component(first, 0) * component(second, 0) + component(first, 1) * component(second, 1) + component(first, 2) * component(second, 2)
    offdiag = component(first, 3) * component(second, 3) + component(first, 4) * component(second, 4) + component(first, 5) * component(second, 5)
    return diagonal + 2.0 * offdiag

def effective_viscosity(rates, factor, exponent, yields):
    second = 0.5 * double_dot(rates, rates) + rate_offset
    creep_part = factor * jnp.power(second, (1.0 - exponent) / (2.0 * exponent))
    plastic = 0.5 * yields * lax.rsqrt(second)
    total_part = creep_part + plastic
    viscosity = creep_part * plastic / total_part + viscosity_least
    creep_slope = creep_part * (1.0 - exponent) / (2.0 * exponent * second)
    plastic_slope = -plastic / (2.0 * second)
    derivative = (plastic * plastic * creep_slope + creep_part * creep_part * plastic_slope) / (total_part * total_part)
    return (viscosity, derivative)

def spread_cells(values):
    return jnp.expand_dims(values, values.ndim - 3)

def divergence(padded):
    return jnp.stack([centered(component(padded, tensor_slots[i][0]), 0) + centered(component(padded, tensor_slots[i][1]), 1) + centered(component(padded, tensor_slots[i][2]), 2) for i in range(3)], axis=-4)

def tangent_stress(viscosity, derivative, rates, change):
    return 2.0 * spread_cells(viscosity) * change + 2.0 * spread_cells(derivative * double_dot(rates, change)) * rates

def phase_params(phase_ids, creep_factor, stress_exponent, yield_stress):
    choose = (phase_ids[None] == jnp.arange(creep_factor.shape[0], dtype=jnp.int32)[:, None, None, None]).astype(jnp.float32)
    return tuple((lax.optimization_barrier(jnp.sum(choose * entries[:, None, None, None], axis=0)) for entries in (creep_factor, stress_exponent, yield_stress)))

def pad_cells(values):
    return jnp.pad(values, [(0, 0)] * (values.ndim - 3) + [(1, 1)] * 3)

def reference(velocity, direction, pressure, body_force, phase_ids, creep_factor, stress_exponent, yield_stress, accepted):
    factor, exponent, yields = phase_params(phase_ids, creep_factor, stress_exponent, yield_stress)
    padded_pressure = pad_cells(pressure)
    loading = body_force - jnp.stack([centered(padded_pressure, j) for j in range(3)])
    base_rates = strain_rates(pad_cells(velocity))
    base_viscosity, base_slope = effective_viscosity(base_rates, factor, exponent, yields)
    residual_base = divergence(pad_cells(2.0 * spread_cells(base_viscosity) * base_rates)) + loading
    change_rates = strain_rates(pad_cells(direction))
    jacobian = divergence(pad_cells(tangent_stress(base_viscosity, base_slope, base_rates, change_rates)))
    cells = 3.0 * velocity.shape[1] * velocity.shape[2] * velocity.shape[3]
    actual = []
    predicted = []
    chosen_velocity = jnp.zeros_like(velocity)
    chosen_residual = jnp.zeros_like(velocity)
    for number, length in enumerate(step_lengths):
        trial_velocity = velocity + length * direction
        trial_rates = strain_rates(pad_cells(trial_velocity))
        trial_viscosity, unused_slope = effective_viscosity(trial_rates, factor, exponent, yields)
        trial_residual = divergence(pad_cells(2.0 * spread_cells(trial_viscosity) * trial_rates)) + loading
        linear = residual_base + length * jacobian
        actual.append(jnp.sum(trial_residual * trial_residual))
        predicted.append(jnp.sum(linear * linear))
        picked = accepted[0] == number
        chosen_velocity = jnp.where(picked, trial_velocity, chosen_velocity)
        chosen_residual = jnp.where(picked, trial_residual, chosen_residual)
    sums = jnp.stack(actual + predicted)
    norms = jnp.sqrt(sums / cells + tiny_mean).reshape(2, 4)
    return (norms, chosen_velocity, chosen_residual)
```

```python
import functools

import jax
import jax.numpy as jnp
from jax import lax
from jax.experimental import pallas as pl
from jax.experimental.pallas import tpu as pltpu
from jax.sharding import PartitionSpec as P

MESH = pl.DeviceIdType.MESH
LENGTHS = (1.0, 0.5, 0.25, 0.125)
ROWS = 24
TOP = 8
ALONG = ((0, 3, 4), (3, 1, 5), (4, 5, 2))


def roll(values, shift, axis):
    return pltpu.roll(values, shift % values.shape[axis], axis)


def kernel(
    sizes,
    v_hbm, d_hbm, p_hbm, b_hbm, ph_hbm, fac_ref, exp_ref, yld_ref, acc_ref,
    norms_ref, cv_hbm, cr_hbm,
    VP, PP, HP, BF, YS, YR, WS, ZR, XZ, YZ, ES, ER, SS, CV, CR, RZ, RX, RY,
    load_sem, out_sem, send_sem, recv_sem, rz_sem, rx_sem, ry_sem,
):
    n = dict(zip(("gx", "gy", "gz"), sizes))
    me = {a: lax.axis_index(a) for a in n}
    has = {}
    for a in n:
        has[a, 1] = me[a] < n[a] - 1
        has[a, -1] = me[a] > 0
    f32 = jnp.float32
    lane = lax.broadcasted_iota(jnp.int32, (8, 128), 1)
    sub = lax.broadcasted_iota(jnp.int32, (8, 128), 0)
    odd = (lane & 1) == 1
    first_lane, last_lane = lane == 0, lane == 127

    block = pl.ds(TOP, 8)
    loads = [
        pltpu.make_async_copy(v_hbm, VP.at[pl.ds(0, 3), pl.ds(2, 8), block], load_sem.at[0]),
        pltpu.make_async_copy(d_hbm, VP.at[pl.ds(3, 3), pl.ds(2, 8), block], load_sem.at[1]),
        pltpu.make_async_copy(p_hbm, PP.at[pl.ds(1, 8), block], load_sem.at[2]),
        pltpu.make_async_copy(ph_hbm, HP.at[pl.ds(1, 8)], load_sem.at[3]),
        pltpu.make_async_copy(b_hbm, BF, load_sem.at[4]),
    ]
    for load in loads:
        load.start()

    zero = jnp.zeros((8, 128), f32)
    for c in range(6):
        for x in (0, 1, 10, 11):
            VP[c, x, block] = zero
    for x in (0, 9):
        PP[x, block] = zero
        HP[x] = jnp.zeros((8, 128), jnp.int32)
    for ref in (YR, ZR, XZ, YZ, ER):
        ref[...] = jnp.zeros(ref.shape, f32)

    counter = [0]

    def message(step, pairs):
        send = functools.reduce(jnp.logical_and, [has[a, s] for a, s in step.items()])
        recv = functools.reduce(jnp.logical_and, [has[a, -s] for a, s in step.items()])
        target = {a: me[a] + s for a, s in step.items()}
        copies = []
        for src, dst in pairs:
            i = counter[0]
            counter[0] += 1
            copies.append(
                pltpu.make_async_remote_copy(
                    src_ref=src, dst_ref=dst, send_sem=send_sem.at[i], recv_sem=recv_sem.at[i],
                    device_id=target, device_id_type=MESH,
                )
            )
        return send, recv, copies

    def start(messages):
        for send, _, copies in messages:
            @pl.when(send)
            def _():
                for copy in copies:
                    copy.start()

    def arrived(messages):
        for _, recv, copies in messages:
            @pl.when(recv)
            def _():
                for copy in copies:
                    copy.wait_recv()

    def sent(messages):
        for send, _, copies in messages:
            @pl.when(send)
            def _():
                for copy in copies:
                    copy.wait_send()

    both = (1, -1)
    hi = lambda s: (s + 1) // 2
    lo = lambda s: (1 - s) // 2
    x_near, x_far, y_near, y_far, z_face, xz_edge, yz_edge, xy_edge = ([] for _ in range(8))
    for s in both:
        near_from, near_to = (9, 1) if s == 1 else (2, 10)
        far_from, far_to = (8, 0) if s == 1 else (3, 11)
        p_from, p_to = (8, 0) if s == 1 else (1, 9)
        x_near.append(message({"gx": s}, [
            (VP.at[:, near_from, block], VP.at[:, near_to, block]),
            (PP.at[p_from, block], PP.at[p_to, block]),
        ]))
        x_far.append(message({"gx": s}, [
            (VP.at[:, far_from, block], VP.at[:, far_to, block]),
            (HP.at[p_from], HP.at[p_to]),
        ]))
        y_near.append(message({"gy": s}, [(YS.at[hi(s), pl.ds(0, 7)], YR.at[lo(s), pl.ds(0, 7)])]))
        y_far.append(message({"gy": s}, [(YS.at[hi(s), pl.ds(7, 7)], YR.at[lo(s), pl.ds(7, 7)])]))
        z_face.append(message({"gz": s}, [(WS.at[pl.ds(0, 2)], ZR.at[lo(s)])]))
        for t in both:
            xz_edge.append(message({"gx": s, "gz": t}, [(WS.at[pl.ds(1, 1)], XZ.at[lo(s), lo(t)])]))
            yz_edge.append(message({"gy": s, "gz": t}, [(WS.at[pl.ds(1, 2)], YZ.at[lo(s), lo(t)])]))
            xy_edge.append(message({"gx": s, "gy": t}, [(ES.at[hi(s), hi(t)], ER.at[lo(s), lo(t)])]))

    barrier = pltpu.get_barrier_semaphore()
    for a in n:
        for k in range(1, n[a]):
            pl.semaphore_signal(barrier, inc=1, device_id={a: lax.rem(me[a] + k, n[a])}, device_id_type=MESH)
    for a, b in (("gx", "gy"), ("gx", "gz"), ("gy", "gz")):
        for s in both:
            for t in both:
                @pl.when(jnp.logical_and(has[a, s], has[b, t]))
                def _():
                    pl.semaphore_signal(
                        barrier, inc=1, device_id={a: me[a] + s, b: me[b] + t}, device_id_type=MESH
                    )
    sides = {a: has[a, 1].astype(jnp.int32) + has[a, -1].astype(jnp.int32) for a in n}
    edges = sides["gx"] * sides["gy"] + sides["gx"] * sides["gz"] + sides["gy"] * sides["gz"]

    for load in loads[:4]:
        load.wait()

    def y_layer(c, y):
        return VP[c, pl.ds(2, 8), TOP + y]

    for side, near, far in ((0, 0, 1), (1, 7, 6)):
        for c in range(6):
            YS[side, c] = y_layer(c, near)
            YS[side, 8 + c] = y_layer(c, far)
        YS[side, 6] = PP[pl.ds(1, 8), TOP + near]
        YS[side, 7] = HP[pl.ds(1, 8), near, :].astype(f32)
        for s, xp in ((0, 2), (1, 9)):
            for c in range(6):
                ES[s, side, pl.ds(c, 1)] = VP[c, xp, pl.ds(TOP + near, 1)]

    pair = lane >> 1
    outer = jnp.where(odd, (lane + 1) >> 1, (lane >> 1) - 1) & 63
    near_z, far_z = zero, zero
    for c in range(8):
        one, two = zero, zero
        for x in range(8):
            if c < 6:
                plane = VP[c, x + 2, block]
            elif c == 6:
                plane = PP[x + 1, block]
            else:
                plane = HP[x + 1].astype(f32)
            k = 8 * c + x
            turned = roll(plane, 2 * k + 1, 1)
            one = jnp.where(pair == k, turned, one)
            if c < 6:
                two = jnp.where(outer == k, turned, two)
        near_z = jnp.where((lane >> 4) == c, one, near_z)
        if c < 6:
            far_z = jnp.where((outer >> 3) == c, two, far_z)
    WS[0] = far_z
    WS[1] = near_z
    near_zy = zero
    for side in range(2):
        for c in range(6):
            k = 8 * side + c
            near_zy = jnp.where(pair == k, roll(YS[side, c], 2 * k + 1, 1), near_zy)
    WS[2] = near_zy

    pl.semaphore_wait(barrier, sum(n.values()) - 3 + edges)
    for group in (x_near, y_near, z_face, xy_edge, xz_edge, yz_edge, x_far, y_far):
        start(group)

    picked = acc_ref[0]
    length = jnp.where(
        picked == 0, f32(1.0), jnp.where(picked == 1, f32(0.5), jnp.where(picked == 2, f32(0.25), f32(0.125)))
    )
    for c in range(3):
        for x in range(8):
            CV[c, x] = VP[c, x + 2, block] + length * VP[3 + c, x + 2, block]
    out_v = pltpu.make_async_copy(CV, cv_hbm, out_sem.at[0])
    out_v.start()

    full = lambda s: jnp.full((8, 128), s, f32)
    table = []
    for k in range(4):
        exponent = full(exp_ref[k])
        table.append((full(fac_ref[k]), (1.0 - exponent) / (2.0 * exponent), full(0.5 * yld_ref[k])))

    def params(ids):
        out = table[3]
        for k in (2, 1, 0):
            hit = ids == k
            out = tuple(jnp.where(hit, mine, other) for mine, other in zip(table[k], out))
        return out

    def tensor(g):
        return (
            g[0][0], g[1][1], g[2][2],
            0.5 * (g[0][1] + g[1][0]), 0.5 * (g[0][2] + g[2][0]), 0.5 * (g[1][2] + g[2][1]),
        )

    def dot(a, b):
        return (a[0] * b[0] + a[1] * b[1] + a[2] * b[2]) + 2.0 * (a[3] * b[3] + a[4] * b[4] + a[5] * b[5])

    def flow(second, factor, power, half_yield):
        inverse = lax.rsqrt(second)
        creep = factor * jnp.exp(power * jnp.log(second))
        plastic = half_yield * inverse
        total = creep + plastic
        return inverse, creep, plastic, total, creep * plastic / total

    def stresses(g, ids, wanted, mask=None):
        factor, power, half_yield = params(ids)
        base, change = tensor(g[:3]), tensor(g[3:])
        inverse, creep, plastic, total, harmonic = flow(0.125 * dot(base, base) + 0.01, factor, power, half_yield)
        viscosity = harmonic + 0.05
        slope = harmonic * (inverse * inverse) * (plastic * power - 0.5 * creep) / total
        along = slope * (0.25 * dot(base, change))
        if mask is not None:
            viscosity, along = viscosity * mask, along * mask
        fields = [
            {c: viscosity * base[c] for c in wanted},
            {c: viscosity * change[c] + along * base[c] for c in wanted},
        ]
        for a in LENGTHS:
            trial = tuple(e + f if a == 1.0 else e + a * f for e, f in zip(base, change))
            viscosity = flow(0.125 * dot(trial, trial) + 0.01, factor, power, half_yield)[4] + 0.05
            if mask is not None:
                viscosity = viscosity * mask
            fields.append({c: viscosity * trial[c] for c in wanted})
        return fields

    def across_z(plane, ends):
        return jnp.where(last_lane, ends, roll(plane, -1, 1)) - jnp.where(first_lane, ends, roll(plane, 1, 1))

    def ends_of(packed, k):
        return roll(packed, -(2 * k + 1), 1)

    def joined(below, above):
        return jnp.where(odd, roll(below, 1, 1), roll(above, -1, 1))

    def flag(a, s):
        return has[a, s].astype(f32)

    def plane_differences(xp, packed, x):
        g = []
        for c in range(6):
            centre = VP[c, xp, block]
            g.append((
                VP[c, xp + 1, block] - VP[c, xp - 1, block],
                VP[c, xp, pl.ds(TOP + 1, 8)] - VP[c, xp, pl.ds(TOP - 1, 8)],
                across_z(centre, ends_of(packed, 8 * c + x)),
            ))
        return g

    every = tuple(range(6))

    def store_plane(xs, fields):
        for f, field in enumerate(fields):
            for c, value in field.items():
                SS[f, c, xs, block] = value

    arrived(z_face)
    arrived(y_near)
    near_halo = joined(ZR[0, 1], ZR[1, 1])
    far_halo = jnp.where(odd, roll(ZR[0, 0], 2, 1), roll(ZR[1, 0], -2, 1))
    for side, row in ((0, TOP - 1), (1, TOP + 8)):
        for c in range(6):
            VP[c, pl.ds(2, 8), row] = YR[side, c]
        PP[pl.ds(1, 8), row] = YR[side, 6]
    for x in range(1, 7):
        store_plane(x + 1, stresses(plane_differences(x + 2, near_halo, x), HP[x + 1], every))

    arrived(x_near)
    for x in (0, 7):
        store_plane(x + 1, stresses(plane_differences(x + 2, near_halo, x), HP[x + 1], every))
    arrived(xy_edge)
    arrived(xz_edge)
    x_ends = [joined(XZ[side, 0, 0], XZ[side, 1, 0]) for side in range(2)]
    for s, xp in ((0, 1), (1, 10)):
        for t, row in ((0, TOP - 1), (1, TOP + 8)):
            for c in range(6):
                VP[c, xp, pl.ds(row, 1)] = ER[s, t, pl.ds(c, 1)]
    arrived(x_far)
    for side, xp, x in ((0, 1, 7), (1, 10, 0)):
        g = plane_differences(xp, x_ends[side], x)
        store_plane(xp - 1, stresses(g, HP[xp - 1], ALONG[0], flag("gx", 2 * side - 1)))

    arrived(yz_edge)
    arrived(y_far)
    for side in range(2):
        packed = joined(YZ[side, 0, 1], YZ[side, 1, 1])
        g = []
        for c in range(6):
            centre = YR[side, c]
            above = jnp.where(sub == 7, ER[1, side, pl.ds(c, 1)], roll(centre, -1, 0))
            below = jnp.where(sub == 0, ER[0, side, pl.ds(c, 1)], roll(centre, 1, 0))
            outward = YS[side, c] - YR[side, 8 + c]
            g.append((
                above - below,
                outward if side == 0 else -outward,
                across_z(centre, ends_of(packed, 8 * (1 - side) + c)),
            ))
        fields = stresses(g, YR[side, 7], ALONG[1], flag("gy", 2 * side - 1))
        row = TOP - 1 if side == 0 else TOP + 8
        for f, field in enumerate(fields):
            for c, value in field.items():
                SS[f, c, pl.ds(1, 8), row] = value

    inner = WS[1]
    y_ends = [joined(YZ[side, 0, 0], YZ[side, 1, 0]) for side in range(2)]
    column = pair & 7
    out_z = jnp.where(odd, inner - far_halo, far_halo - inner)
    out_y = roll(jnp.where(sub == 0, y_ends[1], near_halo), -1, 0) - roll(
        jnp.where(sub == 7, y_ends[0], near_halo), 1, 0
    )
    out_x = jnp.where(column == 7, roll(x_ends[1], 14, 1), roll(near_halo, -2, 1)) - jnp.where(
        column == 0, roll(x_ends[0], -14, 1), roll(near_halo, 2, 1)
    )
    g = [tuple(roll(o, -16 * c, 1) if c else o for o in (out_x, out_y, out_z)) for c in range(6)]
    mask = jnp.where(odd, flag("gz", -1), flag("gz", 1))
    z_fields = stresses(g, roll(near_halo, -112, 1), ALONG[2], mask)

    loads[4].wait()
    sums = [zero] * 8
    for x in range(8):
        xs = x + 1
        p_plane = PP[xs, block]
        slope = (
            PP[xs + 1, block] - PP[xs - 1, block],
            PP[xs, pl.ds(TOP + 1, 8)] - PP[xs, pl.ds(TOP - 1, 8)],
            across_z(p_plane, ends_of(near_halo, 48 + x)),
        )
        for i in range(3):
            loading = BF[i, x] - 0.5 * slope[i]
            cx, cy, cz = ALONG[0][i], ALONG[1][i], ALONG[2][i]
            out = []
            for f in range(6):
                change = SS[f, cx, xs + 1, block] - SS[f, cx, xs - 1, block]
                change = change + (SS[f, cy, xs, pl.ds(TOP + 1, 8)] - SS[f, cy, xs, pl.ds(TOP - 1, 8)])
                change = change + across_z(SS[f, cz, xs, block], ends_of(z_fields[f][cz], x))
                out.append(0.5 * change if f == 1 else 0.5 * change + loading)
            chosen = out[5]
            for k in (2, 1, 0):
                chosen = jnp.where(picked == k, out[2 + k], chosen)
            CR[i, x] = chosen
            for k, a in enumerate(LENGTHS):
                sums[k] = sums[k] + out[2 + k] * out[2 + k]
                linear = out[0] + a * out[1]
                sums[4 + k] = sums[4 + k] + linear * linear
    out_r = pltpu.make_async_copy(CR, cr_hbm, out_sem.at[1])
    out_r.start()

    stacked = zero
    for k in range(8):
        stacked = jnp.where(sub == k, jnp.sum(sums[k], axis=0, keepdims=True), stacked)
    totals = jnp.sum(stacked, axis=1, keepdims=True)
    row = jnp.sum(jnp.where(lane == sub, totals, 0.0), axis=0, keepdims=True)
    shares = []
    for a, ref, sems in (("gz", RZ, rz_sem), ("gx", RX, rx_sem), ("gy", RY, ry_sem)):
        mine = me[a]
        ref[mine] = row
        copies = []
        for k in range(1, n[a]):
            copies.append(
                pltpu.make_async_remote_copy(
                    src_ref=ref.at[mine], dst_ref=ref.at[mine], send_sem=sems.at[0, k], recv_sem=sems.at[1, k],
                    device_id={a: lax.rem(mine + k, n[a])}, device_id_type=MESH,
                )
            )
        for copy in copies:
            copy.start()
        for copy in copies:
            copy.wait_recv()
        row = ref[0]
        for k in range(1, n[a]):
            row = row + ref[k]
        shares += copies
    cells = 3.0 * (8 * n["gx"]) * (8 * n["gy"]) * (128 * n["gz"])
    norms = jnp.sqrt(row / cells + 1e-6)
    norms_ref[pl.ds(0, 1)] = norms[:, 0:4]
    norms_ref[pl.ds(1, 1)] = roll(jnp.broadcast_to(norms, (8, 128)), -4, 1)[0:1, 0:4]

    for copy in shares:
        copy.wait_send()
    for group in (x_near, y_near, z_face, xy_edge, xz_edge, yz_edge, x_far, y_far):
        sent(group)
    out_v.wait()
    out_r.wait()


def solution(mesh):
    sizes = tuple(mesh.shape[a] for a in ("gx", "gy", "gz"))
    f32 = jnp.float32

    def body(*args):
        vector = jax.ShapeDtypeStruct((3, 8, 8, 128), f32)
        anywhere = pl.BlockSpec(memory_space=pl.ANY)
        scalars = pl.BlockSpec(memory_space=pltpu.SMEM)
        return pl.pallas_call(
            functools.partial(kernel, sizes),
            out_shape=(jax.ShapeDtypeStruct((2, 4), f32), vector, vector),
            in_specs=[anywhere] * 5 + [scalars] * 4,
            out_specs=(pl.BlockSpec(memory_space=pltpu.VMEM), anywhere, anywhere),
            scratch_shapes=[
                pltpu.VMEM((6, 12, ROWS, 128), f32),
                pltpu.VMEM((10, ROWS, 128), f32),
                pltpu.VMEM((10, 8, 128), jnp.int32),
                pltpu.VMEM((3, 8, 8, 128), f32),
                pltpu.VMEM((2, 14, 8, 128), f32),
                pltpu.VMEM((2, 14, 8, 128), f32),
                pltpu.VMEM((3, 8, 128), f32),
                pltpu.VMEM((2, 2, 8, 128), f32),
                pltpu.VMEM((2, 2, 1, 8, 128), f32),
                pltpu.VMEM((2, 2, 2, 8, 128), f32),
                pltpu.VMEM((2, 2, 8, 128), f32),
                pltpu.VMEM((2, 2, 8, 128), f32),
                pltpu.VMEM((6, 6, 10, ROWS, 128), f32),
                pltpu.VMEM((3, 8, 8, 128), f32),
                pltpu.VMEM((3, 8, 8, 128), f32),
                pltpu.VMEM((sizes[2], 1, 128), f32),
                pltpu.VMEM((sizes[0], 1, 128), f32),
                pltpu.VMEM((sizes[1], 1, 128), f32),
                pltpu.SemaphoreType.DMA((5,)),
                pltpu.SemaphoreType.DMA((2,)),
                pltpu.SemaphoreType.DMA((26,)),
                pltpu.SemaphoreType.DMA((26,)),
                pltpu.SemaphoreType.DMA((2, sizes[2])),
                pltpu.SemaphoreType.DMA((2, sizes[0])),
                pltpu.SemaphoreType.DMA((2, sizes[1])),
            ],
            compiler_params=pltpu.CompilerParams(collective_id=0, has_side_effects=True),
            name="line_search",
        )(*args)

    vector, scalar = P(None, "gx", "gy", "gz"), P("gx", "gy", "gz")
    return jax.shard_map(
        body,
        mesh=mesh,
        in_specs=(vector, vector, scalar, vector, scalar, P(), P(), P(), P()),
        out_specs=(P(), vector, vector),
        check_vma=False,
    )
```

```python
import functools

import jax
import jax.numpy as jnp
from jax import lax
from jax.experimental import pallas as pl
from jax.experimental.pallas import tpu as pltpu
from jax.sharding import PartitionSpec as P

MESH = pl.DeviceIdType.MESH
LENGTHS = (1.0, 0.5, 0.25, 0.125)
ROWS = 24
TOP = 8
ALONG = ((0, 3, 4), (3, 1, 5), (4, 5, 2))


def roll(values, shift, axis):
    return pltpu.roll(values, shift % values.shape[axis], axis)


def kernel(
    sizes,
    v_hbm, d_hbm, p_hbm, b_hbm, ph_hbm, fac_hbm, exp_hbm, yld_hbm, acc_ref,
    norms_ref, CV, CR,
    fac_ref, exp_ref, yld_ref, VP, PP, HP, BF, YS, YR, WS, ZR, XZ, YZ, ES, ER, SS, RZ, RX, RY,
    load_sem, send_sem, recv_sem, rz_sem, rx_sem, ry_sem,
):
    n = dict(zip(("gx", "gy", "gz"), sizes))
    me = {a: lax.axis_index(a) for a in n}
    has = {}
    for a in n:
        has[a, 1] = me[a] < n[a] - 1
        has[a, -1] = me[a] > 0
    f32 = jnp.float32
    lane = lax.broadcasted_iota(jnp.int32, (8, 128), 1)
    sub = lax.broadcasted_iota(jnp.int32, (8, 128), 0)
    odd = (lane & 1) == 1
    first_lane, last_lane = lane == 0, lane == 127

    block = pl.ds(TOP, 8)
    loads = [
        pltpu.make_async_copy(v_hbm, VP.at[pl.ds(0, 3), pl.ds(2, 8), block], load_sem.at[0]),
        pltpu.make_async_copy(d_hbm, VP.at[pl.ds(3, 3), pl.ds(2, 8), block], load_sem.at[1]),
        pltpu.make_async_copy(p_hbm, PP.at[pl.ds(1, 8), block], load_sem.at[2]),
        pltpu.make_async_copy(ph_hbm, HP.at[pl.ds(1, 8)], load_sem.at[3]),
        pltpu.make_async_copy(b_hbm, BF, load_sem.at[4]),
        pltpu.make_async_copy(fac_hbm, fac_ref, load_sem.at[5]),
        pltpu.make_async_copy(exp_hbm, exp_ref, load_sem.at[6]),
        pltpu.make_async_copy(yld_hbm, yld_ref, load_sem.at[7]),
    ]
    for load in loads:
        load.start()

    zero = jnp.zeros((8, 128), f32)
    for c in range(6):
        for x in (0, 1, 10, 11):
            VP[c, x, block] = zero
    for x in (0, 9):
        PP[x, block] = zero
        HP[x] = jnp.zeros((8, 128), jnp.int32)
    for ref in (YR, ZR, XZ, YZ, ER):
        ref[...] = jnp.zeros(ref.shape, f32)

    counter = [0]

    def message(step, pairs):
        send = functools.reduce(jnp.logical_and, [has[a, s] for a, s in step.items()])
        recv = functools.reduce(jnp.logical_and, [has[a, -s] for a, s in step.items()])
        target = {a: me[a] + s for a, s in step.items()}
        copies = []
        for src, dst in pairs:
            i = counter[0]
            counter[0] += 1
            copies.append(
                pltpu.make_async_remote_copy(
                    src_ref=src, dst_ref=dst, send_sem=send_sem.at[i], recv_sem=recv_sem.at[i],
                    device_id=target, device_id_type=MESH,
                )
            )
        return send, recv, copies

    def start(messages):
        for send, _, copies in messages:
            @pl.when(send)
            def _():
                for copy in copies:
                    copy.start()

    def arrived(messages):
        for _, recv, copies in messages:
            @pl.when(recv)
            def _():
                for copy in copies:
                    copy.wait_recv()

    def sent(messages):
        for send, _, copies in messages:
            @pl.when(send)
            def _():
                for copy in copies:
                    copy.wait_send()

    both = (1, -1)
    hi = lambda s: (s + 1) // 2
    lo = lambda s: (1 - s) // 2
    x_near, x_far, y_near, y_far, z_face, xz_edge, yz_edge, xy_edge = ([] for _ in range(8))
    for s in both:
        near_from, near_to = (9, 1) if s == 1 else (2, 10)
        far_from, far_to = (8, 0) if s == 1 else (3, 11)
        p_from, p_to = (8, 0) if s == 1 else (1, 9)
        x_near.append(message({"gx": s}, [
            (VP.at[:, near_from, block], VP.at[:, near_to, block]),
            (PP.at[p_from, block], PP.at[p_to, block]),
        ]))
        x_far.append(message({"gx": s}, [
            (VP.at[:, far_from, block], VP.at[:, far_to, block]),
            (HP.at[p_from], HP.at[p_to]),
        ]))
        y_near.append(message({"gy": s}, [(YS.at[hi(s), pl.ds(0, 7)], YR.at[lo(s), pl.ds(0, 7)])]))
        y_far.append(message({"gy": s}, [(YS.at[hi(s), pl.ds(7, 7)], YR.at[lo(s), pl.ds(7, 7)])]))
        z_face.append(message({"gz": s}, [(WS.at[pl.ds(0, 2)], ZR.at[lo(s)])]))
        for t in both:
            xz_edge.append(message({"gx": s, "gz": t}, [(WS.at[pl.ds(1, 1)], XZ.at[lo(s), lo(t)])]))
            yz_edge.append(message({"gy": s, "gz": t}, [(WS.at[pl.ds(1, 2)], YZ.at[lo(s), lo(t)])]))
            xy_edge.append(message({"gx": s, "gy": t}, [(ES.at[hi(s), hi(t)], ER.at[lo(s), lo(t)])]))

    barrier = pltpu.get_barrier_semaphore()
    for a, b in (("gx", "gy"), ("gx", "gz"), ("gy", "gz")):
        for s in both:
            for t in both:
                @pl.when(jnp.logical_and(has[a, s], has[b, t]))
                def _():
                    pl.semaphore_signal(
                        barrier, inc=1, device_id={a: me[a] + s, b: me[b] + t}, device_id_type=MESH
                    )
    for a in n:
        for k in sorted(range(1, n[a]), key=lambda k: min(k, n[a] - k)):
            pl.semaphore_signal(barrier, inc=1, device_id={a: lax.rem(me[a] + k, n[a])}, device_id_type=MESH)
    sides = {a: has[a, 1].astype(jnp.int32) + has[a, -1].astype(jnp.int32) for a in n}
    edges = sides["gx"] * sides["gy"] + sides["gx"] * sides["gz"] + sides["gy"] * sides["gz"]

    for load in loads[:4]:
        load.wait()

    def y_layer(c, y):
        return VP[c, pl.ds(2, 8), TOP + y]

    for side, near, far in ((0, 0, 1), (1, 7, 6)):
        for c in range(6):
            YS[side, c] = y_layer(c, near)
            YS[side, 8 + c] = y_layer(c, far)
        YS[side, 6] = PP[pl.ds(1, 8), TOP + near]
        YS[side, 7] = HP[pl.ds(1, 8), near, :].astype(f32)
        for s, xp in ((0, 2), (1, 9)):
            for c in range(6):
                ES[s, side, pl.ds(c, 1)] = VP[c, xp, pl.ds(TOP + near, 1)]

    pair = lane >> 1
    outer = jnp.where(odd, (lane + 1) >> 1, (lane >> 1) - 1) & 63
    near_z, far_z = zero, zero
    for c in range(8):
        one, two = zero, zero
        for x in range(8):
            if c < 6:
                plane = VP[c, x + 2, block]
            elif c == 6:
                plane = PP[x + 1, block]
            else:
                plane = HP[x + 1].astype(f32)
            k = 8 * c + x
            turned = roll(plane, 2 * k + 1, 1)
            one = jnp.where(pair == k, turned, one)
            if c < 6:
                two = jnp.where(outer == k, turned, two)
        near_z = jnp.where((lane >> 4) == c, one, near_z)
        if c < 6:
            far_z = jnp.where((outer >> 3) == c, two, far_z)
    WS[0] = far_z
    WS[1] = near_z
    near_zy = zero
    for side in range(2):
        for c in range(6):
            k = 8 * side + c
            near_zy = jnp.where(pair == k, roll(YS[side, c], 2 * k + 1, 1), near_zy)
    WS[2] = near_zy

    pl.semaphore_wait(barrier, sum(n.values()) - 3 + edges)
    for group in (x_near, y_near, z_face, xy_edge, xz_edge, yz_edge, x_far, y_far):
        start(group)

    for load in loads[5:]:
        load.wait()
    picked = acc_ref[0]
    length = jnp.where(
        picked == 0, f32(1.0), jnp.where(picked == 1, f32(0.5), jnp.where(picked == 2, f32(0.25), f32(0.125)))
    )
    for c in range(3):
        for x in range(8):
            CV[c, x] = VP[c, x + 2, block] + length * VP[3 + c, x + 2, block]

    full = lambda s: jnp.full((8, 128), s, f32)
    table = []
    for k in range(4):
        exponent = full(exp_ref[k])
        table.append((full(fac_ref[k]), (1.0 - exponent) / (2.0 * exponent), full(0.5 * yld_ref[k])))

    def params(ids):
        out = table[3]
        for k in (2, 1, 0):
            hit = ids == k
            out = tuple(jnp.where(hit, mine, other) for mine, other in zip(table[k], out))
        return out

    def tensor(g):
        return (
            g[0][0], g[1][1], g[2][2],
            0.5 * (g[0][1] + g[1][0]), 0.5 * (g[0][2] + g[2][0]), 0.5 * (g[1][2] + g[2][1]),
        )

    def dot(a, b):
        return (a[0] * b[0] + a[1] * b[1] + a[2] * b[2]) + 2.0 * (a[3] * b[3] + a[4] * b[4] + a[5] * b[5])

    def flow(second, factor, power, half_yield):
        inverse = lax.rsqrt(second)
        creep = factor * jnp.exp(power * jnp.log(second))
        plastic = half_yield * inverse
        total = creep + plastic
        return inverse, creep, plastic, total, creep * plastic / total

    def stresses(g, ids, wanted, mask=None):
        factor, power, half_yield = params(ids)
        base, change = tensor(g[:3]), tensor(g[3:])
        inverse, creep, plastic, total, harmonic = flow(0.125 * dot(base, base) + 0.01, factor, power, half_yield)
        viscosity = harmonic + 0.05
        slope = harmonic * (inverse * inverse) * (plastic * power - 0.5 * creep) / total
        along = slope * (0.25 * dot(base, change))
        if mask is not None:
            viscosity, along = viscosity * mask, along * mask
        fields = [
            {c: viscosity * base[c] for c in wanted},
            {c: viscosity * change[c] + along * base[c] for c in wanted},
        ]
        for a in LENGTHS:
            trial = tuple(e + f if a == 1.0 else e + a * f for e, f in zip(base, change))
            viscosity = flow(0.125 * dot(trial, trial) + 0.01, factor, power, half_yield)[4] + 0.05
            if mask is not None:
                viscosity = viscosity * mask
            fields.append({c: viscosity * trial[c] for c in wanted})
        return fields

    def across_z(plane, ends):
        return jnp.where(last_lane, ends, roll(plane, -1, 1)) - jnp.where(first_lane, ends, roll(plane, 1, 1))

    def ends_of(packed, k):
        return roll(packed, -(2 * k + 1), 1)

    def joined(below, above):
        return jnp.where(odd, roll(below, 1, 1), roll(above, -1, 1))

    def flag(a, s):
        return has[a, s].astype(f32)

    def plane_differences(xp, packed, x):
        g = []
        for c in range(6):
            centre = VP[c, xp, block]
            g.append((
                VP[c, xp + 1, block] - VP[c, xp - 1, block],
                VP[c, xp, pl.ds(TOP + 1, 8)] - VP[c, xp, pl.ds(TOP - 1, 8)],
                across_z(centre, ends_of(packed, 8 * c + x)),
            ))
        return g

    every = tuple(range(6))

    def store_plane(xs, fields):
        for f, field in enumerate(fields):
            for c, value in field.items():
                SS[f, c, xs, block] = value

    arrived(z_face)
    arrived(y_near)
    near_halo = joined(ZR[0, 1], ZR[1, 1])
    far_halo = jnp.where(odd, roll(ZR[0, 0], 2, 1), roll(ZR[1, 0], -2, 1))
    for side, row in ((0, TOP - 1), (1, TOP + 8)):
        for c in range(6):
            VP[c, pl.ds(2, 8), row] = YR[side, c]
        PP[pl.ds(1, 8), row] = YR[side, 6]
    for x in range(1, 7):
        store_plane(x + 1, stresses(plane_differences(x + 2, near_halo, x), HP[x + 1], every))

    arrived(x_near)
    for x in (0, 7):
        store_plane(x + 1, stresses(plane_differences(x + 2, near_halo, x), HP[x + 1], every))
    arrived(xy_edge)
    arrived(xz_edge)
    x_ends = [joined(XZ[side, 0, 0], XZ[side, 1, 0]) for side in range(2)]
    for s, xp in ((0, 1), (1, 10)):
        for t, row in ((0, TOP - 1), (1, TOP + 8)):
            for c in range(6):
                VP[c, xp, pl.ds(row, 1)] = ER[s, t, pl.ds(c, 1)]
    arrived(x_far)
    for side, xp, x in ((0, 1, 7), (1, 10, 0)):
        g = plane_differences(xp, x_ends[side], x)
        store_plane(xp - 1, stresses(g, HP[xp - 1], ALONG[0], flag("gx", 2 * side - 1)))

    arrived(yz_edge)
    arrived(y_far)
    for side in range(2):
        packed = joined(YZ[side, 0, 1], YZ[side, 1, 1])
        g = []
        for c in range(6):
            centre = YR[side, c]
            above = jnp.where(sub == 7, ER[1, side, pl.ds(c, 1)], roll(centre, -1, 0))
            below = jnp.where(sub == 0, ER[0, side, pl.ds(c, 1)], roll(centre, 1, 0))
            outward = YS[side, c] - YR[side, 8 + c]
            g.append((
                above - below,
                outward if side == 0 else -outward,
                across_z(centre, ends_of(packed, 8 * (1 - side) + c)),
            ))
        fields = stresses(g, YR[side, 7], ALONG[1], flag("gy", 2 * side - 1))
        row = TOP - 1 if side == 0 else TOP + 8
        for f, field in enumerate(fields):
            for c, value in field.items():
                SS[f, c, pl.ds(1, 8), row] = value

    inner = WS[1]
    y_ends = [joined(YZ[side, 0, 0], YZ[side, 1, 0]) for side in range(2)]
    column = pair & 7
    out_z = jnp.where(odd, inner - far_halo, far_halo - inner)
    out_y = roll(jnp.where(sub == 0, y_ends[1], near_halo), -1, 0) - roll(
        jnp.where(sub == 7, y_ends[0], near_halo), 1, 0
    )
    out_x = jnp.where(column == 7, roll(x_ends[1], 14, 1), roll(near_halo, -2, 1)) - jnp.where(
        column == 0, roll(x_ends[0], -14, 1), roll(near_halo, 2, 1)
    )
    g = [tuple(roll(o, -16 * c, 1) if c else o for o in (out_x, out_y, out_z)) for c in range(6)]
    mask = jnp.where(odd, flag("gz", -1), flag("gz", 1))
    z_fields = stresses(g, roll(near_halo, -112, 1), ALONG[2], mask)

    loads[4].wait()
    sums = [zero] * 8
    for x in range(8):
        xs = x + 1
        p_plane = PP[xs, block]
        slope = (
            PP[xs + 1, block] - PP[xs - 1, block],
            PP[xs, pl.ds(TOP + 1, 8)] - PP[xs, pl.ds(TOP - 1, 8)],
            across_z(p_plane, ends_of(near_halo, 48 + x)),
        )
        for i in range(3):
            loading = BF[i, x] - 0.5 * slope[i]
            cx, cy, cz = ALONG[0][i], ALONG[1][i], ALONG[2][i]
            out = []
            for f in range(6):
                change = SS[f, cx, xs + 1, block] - SS[f, cx, xs - 1, block]
                change = change + (SS[f, cy, xs, pl.ds(TOP + 1, 8)] - SS[f, cy, xs, pl.ds(TOP - 1, 8)])
                change = change + across_z(SS[f, cz, xs, block], ends_of(z_fields[f][cz], x))
                out.append(0.5 * change if f == 1 else 0.5 * change + loading)
            chosen = out[5]
            for k in (2, 1, 0):
                chosen = jnp.where(picked == k, out[2 + k], chosen)
            CR[i, x] = chosen
            for k, a in enumerate(LENGTHS):
                sums[k] = sums[k] + out[2 + k] * out[2 + k]
                linear = out[0] + a * out[1]
                sums[4 + k] = sums[4 + k] + linear * linear

    stacked = zero
    for k in range(8):
        stacked = jnp.where(sub == k, jnp.sum(sums[k], axis=0, keepdims=True), stacked)
    totals = jnp.sum(stacked, axis=1, keepdims=True)
    row = jnp.sum(jnp.where(lane == sub, totals, 0.0), axis=0, keepdims=True)
    shares = []
    for a, ref, sems in (("gz", RZ, rz_sem), ("gx", RX, rx_sem), ("gy", RY, ry_sem)):
        mine = me[a]
        ref[mine] = row
        copies = []
        for k in range(1, n[a]):
            copies.append(
                pltpu.make_async_remote_copy(
                    src_ref=ref.at[mine], dst_ref=ref.at[mine], send_sem=sems.at[0, k], recv_sem=sems.at[1, k],
                    device_id={a: lax.rem(mine + k, n[a])}, device_id_type=MESH,
                )
            )
        for copy in copies:
            copy.start()
        for copy in copies:
            copy.wait_recv()
        row = ref[0]
        for k in range(1, n[a]):
            row = row + ref[k]
        shares += copies
    cells = 3.0 * (8 * n["gx"]) * (8 * n["gy"]) * (128 * n["gz"])
    norms = jnp.sqrt(row / cells + 1e-6)
    norms_ref[pl.ds(0, 1)] = norms[:, 0:4]
    norms_ref[pl.ds(1, 1)] = roll(jnp.broadcast_to(norms, (8, 128)), -4, 1)[0:1, 0:4]

    for copy in shares:
        copy.wait_send()
    for group in (x_near, y_near, z_face, xy_edge, xz_edge, yz_edge, x_far, y_far):
        sent(group)


def write_out(*refs):
    copies = [pltpu.make_async_copy(refs[i], refs[3 + i], refs[6].at[i]) for i in range(3)]
    for copy in copies:
        copy.start()
    for copy in copies:
        copy.wait()


def solution(mesh):
    sizes = tuple(mesh.shape[a] for a in ("gx", "gy", "gz"))
    f32 = jnp.float32

    def body(*args):
        vector = jax.ShapeDtypeStruct((3, 8, 8, 128), f32)
        anywhere = pl.BlockSpec(memory_space=pl.ANY)
        inside = pl.BlockSpec(memory_space=pltpu.VMEM)
        args = [pltpu.with_memory_space_constraint(a, pltpu.HBM) for a in args[:8]] + [args[8]]
        outputs = (jax.ShapeDtypeStruct((2, 4), f32), vector, vector)
        found = pl.pallas_call(
            functools.partial(kernel, sizes),
            out_shape=outputs,
            in_specs=[pl.BlockSpec(memory_space=pltpu.HBM)] * 8 + [pl.BlockSpec(memory_space=pltpu.SMEM)],
            out_specs=(inside,) * 3,
            scratch_shapes=[
                pltpu.SMEM((4,), f32),
                pltpu.SMEM((4,), f32),
                pltpu.SMEM((4,), f32),
                pltpu.VMEM((6, 12, ROWS, 128), f32),
                pltpu.VMEM((10, ROWS, 128), f32),
                pltpu.VMEM((10, 8, 128), jnp.int32),
                pltpu.VMEM((3, 8, 8, 128), f32),
                pltpu.VMEM((2, 14, 8, 128), f32),
                pltpu.VMEM((2, 14, 8, 128), f32),
                pltpu.VMEM((3, 8, 128), f32),
                pltpu.VMEM((2, 2, 8, 128), f32),
                pltpu.VMEM((2, 2, 1, 8, 128), f32),
                pltpu.VMEM((2, 2, 2, 8, 128), f32),
                pltpu.VMEM((2, 2, 8, 128), f32),
                pltpu.VMEM((2, 2, 8, 128), f32),
                pltpu.VMEM((6, 6, 10, ROWS, 128), f32),
                pltpu.VMEM((sizes[2], 1, 128), f32),
                pltpu.VMEM((sizes[0], 1, 128), f32),
                pltpu.VMEM((sizes[1], 1, 128), f32),
                pltpu.SemaphoreType.DMA((8,)),
                pltpu.SemaphoreType.DMA((26,)),
                pltpu.SemaphoreType.DMA((26,)),
                pltpu.SemaphoreType.DMA((2, sizes[2])),
                pltpu.SemaphoreType.DMA((2, sizes[0])),
                pltpu.SemaphoreType.DMA((2, sizes[1])),
            ],
            compiler_params=pltpu.CompilerParams(
                collective_id=0, has_side_effects=True, vmem_limit_bytes=16 * 1024 * 1024
            ),
            name="line_search",
        )(*args)
        return pl.pallas_call(
            write_out,
            out_shape=outputs,
            in_specs=[inside] * 3,
            out_specs=(anywhere,) * 3,
            scratch_shapes=[pltpu.SemaphoreType.DMA((3,))],
            compiler_params=pltpu.CompilerParams(vmem_limit_bytes=4 * 1024 * 1024),
            name="write_out",
        )(*found)

    vector, scalar = P(None, "gx", "gy", "gz"), P("gx", "gy", "gz")
    return jax.shard_map(
        body,
        mesh=mesh,
        in_specs=(vector, vector, scalar, vector, scalar, P(), P(), P(), P()),
        out_specs=(P(), vector, vector),
        check_vma=False,
    )
```

```python
import functools

import jax
import jax.numpy as jnp
from jax import lax
from jax.experimental import pallas as pl
from jax.experimental.pallas import tpu as pltpu
from jax.sharding import PartitionSpec as P

MESH = pl.DeviceIdType.MESH
LENGTHS = (1.0, 0.5, 0.25, 0.125)
ROWS = 24
TOP = 8
ALONG = ((0, 3, 4), (3, 1, 5), (4, 5, 2))


def roll(values, shift, axis):
    return pltpu.roll(values, shift % values.shape[axis], axis)


def known_rounds(sizes):
    def steps(size):
        found, step = [], 1
        while step < size // 2:
            found.append(step)
            step *= 2
        return found

    x, y, z = sizes
    chains = ([("gz", k) for k in steps(z)], [("gx", k) for k in steps(x)] + [("gy", 1)] + [("gy", k) for k in steps(y)])
    rounds, counted = [], 0
    for r in range(max(len(c) for c in chains)):
        rounds.append([])
        for c in chains:
            if r < len(c):
                rounds[-1].append((counted,) + c[r])
                counted += 1
    return rounds


def kernel(
    sizes,
    v_hbm, d_hbm, p_hbm, b_hbm, ph_hbm, fac_hbm, exp_hbm, yld_hbm, acc_ref,
    norms_ref, CV, CR,
    fac_ref, exp_ref, yld_ref, VP, PP, HP, BF, YS, YR, WS, ZR, XZ, YZ, ES, ER, SS, RZ, RP,
    load_sem, send_sem, recv_sem, rz_sem, rp_sem, know_sem,
):
    n = dict(zip(("gx", "gy", "gz"), sizes))
    me = {a: lax.axis_index(a) for a in n}
    has = {}
    for a in n:
        has[a, 1] = me[a] < n[a] - 1
        has[a, -1] = me[a] > 0
    f32 = jnp.float32
    lane = lax.broadcasted_iota(jnp.int32, (8, 128), 1)
    sub = lax.broadcasted_iota(jnp.int32, (8, 128), 0)
    odd = (lane & 1) == 1
    first_lane, last_lane = lane == 0, lane == 127

    block = pl.ds(TOP, 8)
    loads = [
        pltpu.make_async_copy(v_hbm, VP.at[pl.ds(0, 3), pl.ds(2, 8), block], load_sem.at[0]),
        pltpu.make_async_copy(d_hbm, VP.at[pl.ds(3, 3), pl.ds(2, 8), block], load_sem.at[1]),
        pltpu.make_async_copy(p_hbm, PP.at[pl.ds(1, 8), block], load_sem.at[2]),
        pltpu.make_async_copy(ph_hbm, HP.at[pl.ds(1, 8)], load_sem.at[3]),
        pltpu.make_async_copy(b_hbm, BF, load_sem.at[4]),
        pltpu.make_async_copy(fac_hbm, fac_ref, load_sem.at[5]),
        pltpu.make_async_copy(exp_hbm, exp_ref, load_sem.at[6]),
        pltpu.make_async_copy(yld_hbm, yld_ref, load_sem.at[7]),
    ]
    for load in loads:
        load.start()

    zero = jnp.zeros((8, 128), f32)
    for c in range(6):
        for x in (0, 1, 10, 11):
            VP[c, x, block] = zero
    for x in (0, 9):
        PP[x, block] = zero
        HP[x] = jnp.zeros((8, 128), jnp.int32)
    for ref in (YR, ZR, XZ, YZ, ER):
        ref[...] = jnp.zeros(ref.shape, f32)

    counter = [0]

    def message(step, pairs):
        send = functools.reduce(jnp.logical_and, [has[a, s] for a, s in step.items()])
        recv = functools.reduce(jnp.logical_and, [has[a, -s] for a, s in step.items()])
        target = {a: me[a] + s for a, s in step.items()}
        copies = []
        for src, dst in pairs:
            i = counter[0]
            counter[0] += 1
            copies.append(
                pltpu.make_async_remote_copy(
                    src_ref=src, dst_ref=dst, send_sem=send_sem.at[i], recv_sem=recv_sem.at[i],
                    device_id=target, device_id_type=MESH,
                )
            )
        return send, recv, copies

    def start(messages):
        for send, _, copies in messages:
            @pl.when(send)
            def _():
                for copy in copies:
                    copy.start()

    def arrived(messages):
        for _, recv, copies in messages:
            @pl.when(recv)
            def _():
                for copy in copies:
                    copy.wait_recv()

    def sent(messages):
        for send, _, copies in messages:
            @pl.when(send)
            def _():
                for copy in copies:
                    copy.wait_send()

    both = (1, -1)
    hi = lambda s: (s + 1) // 2
    lo = lambda s: (1 - s) // 2
    x_near, x_far, y_near, y_far, z_face, xz_edge, yz_edge, xy_edge = ([] for _ in range(8))
    for s in both:
        near_from, near_to = (9, 1) if s == 1 else (2, 10)
        far_from, far_to = (8, 0) if s == 1 else (3, 11)
        p_from, p_to = (8, 0) if s == 1 else (1, 9)
        x_near.append(message({"gx": s}, [
            (VP.at[:, near_from, block], VP.at[:, near_to, block]),
            (PP.at[p_from, block], PP.at[p_to, block]),
        ]))
        x_far.append(message({"gx": s}, [
            (VP.at[:, far_from, block], VP.at[:, far_to, block]),
            (HP.at[p_from], HP.at[p_to]),
        ]))
        y_near.append(message({"gy": s}, [(YS.at[hi(s), pl.ds(0, 7)], YR.at[lo(s), pl.ds(0, 7)])]))
        y_far.append(message({"gy": s}, [(YS.at[hi(s), pl.ds(7, 7)], YR.at[lo(s), pl.ds(7, 7)])]))
        z_face.append(message({"gz": s}, [(WS.at[pl.ds(0, 2)], ZR.at[lo(s)])]))
        for t in both:
            xz_edge.append(message({"gx": s, "gz": t}, [(WS.at[pl.ds(1, 1)], XZ.at[lo(s), lo(t)])]))
            yz_edge.append(message({"gy": s, "gz": t}, [(WS.at[pl.ds(1, 2)], YZ.at[lo(s), lo(t)])]))
            xy_edge.append(message({"gx": s, "gy": t}, [(ES.at[hi(s), hi(t)], ER.at[lo(s), lo(t)])]))

    barrier = pltpu.get_barrier_semaphore()

    def ring(a, step):
        return {a: lax.rem(me[a] + step + n[a], n[a])}

    for a in n:
        for s in both:
            pl.semaphore_signal(barrier, inc=1, device_id=ring(a, s), device_id_type=MESH)
    for a, b in (("gx", "gy"), ("gx", "gz"), ("gy", "gz")):
        for s in both:
            for t in both:
                @pl.when(jnp.logical_and(has[a, s], has[b, t]))
                def _():
                    pl.semaphore_signal(
                        barrier, inc=1, device_id={a: me[a] + s, b: me[b] + t}, device_id_type=MESH
                    )
    sides = {a: has[a, 1].astype(jnp.int32) + has[a, -1].astype(jnp.int32) for a in n}
    edges = sides["gx"] * sides["gy"] + sides["gx"] * sides["gz"] + sides["gy"] * sides["gz"]

    rounds = known_rounds(sizes)

    def tell(r):
        for i, a, step in rounds[r]:
            for s in both:
                pl.semaphore_signal(know_sem.at[i], inc=1, device_id=ring(a, s * step), device_id_type=MESH)

    def told(r):
        for i, _, _ in rounds[r]:
            pl.semaphore_wait(know_sem.at[i], 2)

    def learn(r):
        if r < len(rounds):
            told(r)
            if r + 1 < len(rounds):
                tell(r + 1)

    for load in loads[:4]:
        load.wait()

    def y_layer(c, y):
        return VP[c, pl.ds(2, 8), TOP + y]

    for side, near, far in ((0, 0, 1), (1, 7, 6)):
        for c in range(6):
            YS[side, c] = y_layer(c, near)
            YS[side, 8 + c] = y_layer(c, far)
        YS[side, 6] = PP[pl.ds(1, 8), TOP + near]
        YS[side, 7] = HP[pl.ds(1, 8), near, :].astype(f32)
        for s, xp in ((0, 2), (1, 9)):
            for c in range(6):
                ES[s, side, pl.ds(c, 1)] = VP[c, xp, pl.ds(TOP + near, 1)]

    pair = lane >> 1
    outer = jnp.where(odd, (lane + 1) >> 1, (lane >> 1) - 1) & 63
    near_z, far_z = zero, zero
    for c in range(8):
        one, two = zero, zero
        for x in range(8):
            if c < 6:
                plane = VP[c, x + 2, block]
            elif c == 6:
                plane = PP[x + 1, block]
            else:
                plane = HP[x + 1].astype(f32)
            k = 8 * c + x
            turned = roll(plane, 2 * k + 1, 1)
            one = jnp.where(pair == k, turned, one)
            if c < 6:
                two = jnp.where(outer == k, turned, two)
        near_z = jnp.where((lane >> 4) == c, one, near_z)
        if c < 6:
            far_z = jnp.where((outer >> 3) == c, two, far_z)
    WS[0] = far_z
    WS[1] = near_z
    near_zy = zero
    for side in range(2):
        for c in range(6):
            k = 8 * side + c
            near_zy = jnp.where(pair == k, roll(YS[side, c], 2 * k + 1, 1), near_zy)
    WS[2] = near_zy

    pl.semaphore_wait(barrier, 6 + edges)
    for group in (x_near, y_near, z_face, xy_edge, xz_edge, yz_edge, x_far, y_far):
        start(group)
    if rounds:
        tell(0)

    for load in loads[5:]:
        load.wait()
    picked = acc_ref[0]
    length = jnp.where(
        picked == 0, f32(1.0), jnp.where(picked == 1, f32(0.5), jnp.where(picked == 2, f32(0.25), f32(0.125)))
    )
    for c in range(3):
        for x in range(8):
            CV[c, x] = VP[c, x + 2, block] + length * VP[3 + c, x + 2, block]

    full = lambda s: jnp.full((8, 128), s, f32)
    table = []
    for k in range(4):
        exponent = full(exp_ref[k])
        table.append((full(fac_ref[k]), (1.0 - exponent) / (2.0 * exponent), full(0.5 * yld_ref[k])))

    def params(ids):
        out = table[3]
        for k in (2, 1, 0):
            hit = ids == k
            out = tuple(jnp.where(hit, mine, other) for mine, other in zip(table[k], out))
        return out

    def tensor(g):
        return (
            g[0][0], g[1][1], g[2][2],
            0.5 * (g[0][1] + g[1][0]), 0.5 * (g[0][2] + g[2][0]), 0.5 * (g[1][2] + g[2][1]),
        )

    def dot(a, b):
        return (a[0] * b[0] + a[1] * b[1] + a[2] * b[2]) + 2.0 * (a[3] * b[3] + a[4] * b[4] + a[5] * b[5])

    def flow(second, factor, power, half_yield):
        inverse = lax.rsqrt(second)
        creep = factor * jnp.exp(power * jnp.log(second))
        plastic = half_yield * inverse
        total = creep + plastic
        return inverse, creep, plastic, total, creep * plastic / total

    def stresses(g, ids, wanted, mask=None):
        factor, power, half_yield = params(ids)
        base, change = tensor(g[:3]), tensor(g[3:])
        inverse, creep, plastic, total, harmonic = flow(0.125 * dot(base, base) + 0.01, factor, power, half_yield)
        viscosity = harmonic + 0.05
        slope = harmonic * (inverse * inverse) * (plastic * power - 0.5 * creep) / total
        along = slope * (0.25 * dot(base, change))
        if mask is not None:
            viscosity, along = viscosity * mask, along * mask
        fields = [
            {c: viscosity * base[c] for c in wanted},
            {c: viscosity * change[c] + along * base[c] for c in wanted},
        ]
        for a in LENGTHS:
            trial = tuple(e + f if a == 1.0 else e + a * f for e, f in zip(base, change))
            viscosity = flow(0.125 * dot(trial, trial) + 0.01, factor, power, half_yield)[4] + 0.05
            if mask is not None:
                viscosity = viscosity * mask
            fields.append({c: viscosity * trial[c] for c in wanted})
        return fields

    def across_z(plane, ends):
        return jnp.where(last_lane, ends, roll(plane, -1, 1)) - jnp.where(first_lane, ends, roll(plane, 1, 1))

    def ends_of(packed, k):
        return roll(packed, -(2 * k + 1), 1)

    def joined(below, above):
        return jnp.where(odd, roll(below, 1, 1), roll(above, -1, 1))

    def flag(a, s):
        return has[a, s].astype(f32)

    def plane_differences(xp, packed, x):
        g = []
        for c in range(6):
            centre = VP[c, xp, block]
            g.append((
                VP[c, xp + 1, block] - VP[c, xp - 1, block],
                VP[c, xp, pl.ds(TOP + 1, 8)] - VP[c, xp, pl.ds(TOP - 1, 8)],
                across_z(centre, ends_of(packed, 8 * c + x)),
            ))
        return g

    every = tuple(range(6))

    def store_plane(xs, fields):
        for f, field in enumerate(fields):
            for c, value in field.items():
                SS[f, c, xs, block] = value

    learn(0)
    learn(1)
    arrived(z_face)
    arrived(y_near)
    near_halo = joined(ZR[0, 1], ZR[1, 1])
    far_halo = jnp.where(odd, roll(ZR[0, 0], 2, 1), roll(ZR[1, 0], -2, 1))
    for side, row in ((0, TOP - 1), (1, TOP + 8)):
        for c in range(6):
            VP[c, pl.ds(2, 8), row] = YR[side, c]
        PP[pl.ds(1, 8), row] = YR[side, 6]
    for x in range(1, 7):
        store_plane(x + 1, stresses(plane_differences(x + 2, near_halo, x), HP[x + 1], every))

    learn(2)

    arrived(x_near)
    for x in (0, 7):
        store_plane(x + 1, stresses(plane_differences(x + 2, near_halo, x), HP[x + 1], every))
    arrived(xy_edge)
    arrived(xz_edge)
    x_ends = [joined(XZ[side, 0, 0], XZ[side, 1, 0]) for side in range(2)]
    for s, xp in ((0, 1), (1, 10)):
        for t, row in ((0, TOP - 1), (1, TOP + 8)):
            for c in range(6):
                VP[c, xp, pl.ds(row, 1)] = ER[s, t, pl.ds(c, 1)]
    arrived(x_far)
    for side, xp, x in ((0, 1, 7), (1, 10, 0)):
        g = plane_differences(xp, x_ends[side], x)
        store_plane(xp - 1, stresses(g, HP[xp - 1], ALONG[0], flag("gx", 2 * side - 1)))

    arrived(yz_edge)
    arrived(y_far)
    for side in range(2):
        packed = joined(YZ[side, 0, 1], YZ[side, 1, 1])
        g = []
        for c in range(6):
            centre = YR[side, c]
            above = jnp.where(sub == 7, ER[1, side, pl.ds(c, 1)], roll(centre, -1, 0))
            below = jnp.where(sub == 0, ER[0, side, pl.ds(c, 1)], roll(centre, 1, 0))
            outward = YS[side, c] - YR[side, 8 + c]
            g.append((
                above - below,
                outward if side == 0 else -outward,
                across_z(centre, ends_of(packed, 8 * (1 - side) + c)),
            ))
        fields = stresses(g, YR[side, 7], ALONG[1], flag("gy", 2 * side - 1))
        row = TOP - 1 if side == 0 else TOP + 8
        for f, field in enumerate(fields):
            for c, value in field.items():
                SS[f, c, pl.ds(1, 8), row] = value

    inner = WS[1]
    y_ends = [joined(YZ[side, 0, 0], YZ[side, 1, 0]) for side in range(2)]
    column = pair & 7
    out_z = jnp.where(odd, inner - far_halo, far_halo - inner)
    out_y = roll(jnp.where(sub == 0, y_ends[1], near_halo), -1, 0) - roll(
        jnp.where(sub == 7, y_ends[0], near_halo), 1, 0
    )
    out_x = jnp.where(column == 7, roll(x_ends[1], 14, 1), roll(near_halo, -2, 1)) - jnp.where(
        column == 0, roll(x_ends[0], -14, 1), roll(near_halo, 2, 1)
    )
    g = [tuple(roll(o, -16 * c, 1) if c else o for o in (out_x, out_y, out_z)) for c in range(6)]
    mask = jnp.where(odd, flag("gz", -1), flag("gz", 1))
    z_fields = stresses(g, roll(near_halo, -112, 1), ALONG[2], mask)

    for r in range(3, len(rounds)):
        learn(r)

    loads[4].wait()
    sums = [zero] * 8
    for x in range(8):
        xs = x + 1
        p_plane = PP[xs, block]
        slope = (
            PP[xs + 1, block] - PP[xs - 1, block],
            PP[xs, pl.ds(TOP + 1, 8)] - PP[xs, pl.ds(TOP - 1, 8)],
            across_z(p_plane, ends_of(near_halo, 48 + x)),
        )
        for i in range(3):
            loading = BF[i, x] - 0.5 * slope[i]
            cx, cy, cz = ALONG[0][i], ALONG[1][i], ALONG[2][i]
            out = []
            for f in range(6):
                change = SS[f, cx, xs + 1, block] - SS[f, cx, xs - 1, block]
                change = change + (SS[f, cy, xs, pl.ds(TOP + 1, 8)] - SS[f, cy, xs, pl.ds(TOP - 1, 8)])
                change = change + across_z(SS[f, cz, xs, block], ends_of(z_fields[f][cz], x))
                out.append(0.5 * change if f == 1 else 0.5 * change + loading)
            chosen = out[5]
            for k in (2, 1, 0):
                chosen = jnp.where(picked == k, out[2 + k], chosen)
            CR[i, x] = chosen
            for k, a in enumerate(LENGTHS):
                sums[k] = sums[k] + out[2 + k] * out[2 + k]
                linear = out[0] + a * out[1]
                sums[4 + k] = sums[4 + k] + linear * linear

    stacked = zero
    for k in range(8):
        stacked = jnp.where(sub == k, jnp.sum(sums[k], axis=0, keepdims=True), stacked)
    totals = jnp.sum(stacked, axis=1, keepdims=True)
    row = jnp.sum(jnp.where(lane == sub, totals, 0.0), axis=0, keepdims=True)
    shares = []
    for axes, ref, sems in ((("gz",), RZ, rz_sem), (("gx", "gy"), RP, rp_sem)):
        offsets = [()]
        for a in axes:
            offsets = [o + (k,) for o in offsets for k in range(n[a])]
        hops = lambda o: sum(min(k, n[a] - k) for k, a in zip(o, axes))
        mine = 0
        for a in axes:
            mine = mine * n[a] + me[a]
        ref[mine] = row
        copies = []
        for i, o in sorted(enumerate(offsets), key=lambda item: -hops(item[1])):
            if any(o):
                copies.append(
                    pltpu.make_async_remote_copy(
                        src_ref=ref.at[mine], dst_ref=ref.at[mine],
                        send_sem=sems.at[0, i], recv_sem=sems.at[1, i],
                        device_id={a: lax.rem(me[a] + k, n[a]) for k, a in zip(o, axes)},
                        device_id_type=MESH,
                    )
                )
        for copy in copies:
            copy.start()
        for copy in copies:
            copy.wait_recv()
        rows = [ref[k] for k in range(len(offsets))]
        while len(rows) > 1:
            rows = [sum(rows[k:k + 2]) for k in range(0, len(rows), 2)]
        row = rows[0]
        shares += copies
    cells = 3.0 * (8 * n["gx"]) * (8 * n["gy"]) * (128 * n["gz"])
    norms = jnp.sqrt(row / cells + 1e-6)
    norms_ref[pl.ds(0, 1)] = norms[:, 0:4]
    norms_ref[pl.ds(1, 1)] = roll(jnp.broadcast_to(norms, (8, 128)), -4, 1)[0:1, 0:4]

    for copy in shares:
        copy.wait_send()
    for group in (x_near, y_near, z_face, xy_edge, xz_edge, yz_edge, x_far, y_far):
        sent(group)


def write_out(*refs):
    copies = [pltpu.make_async_copy(refs[i], refs[3 + i], refs[6].at[i]) for i in range(3)]
    for copy in copies:
        copy.start()
    for copy in copies:
        copy.wait()


def solution(mesh):
    sizes = tuple(mesh.shape[a] for a in ("gx", "gy", "gz"))
    f32 = jnp.float32

    def body(*args):
        vector = jax.ShapeDtypeStruct((3, 8, 8, 128), f32)
        anywhere = pl.BlockSpec(memory_space=pl.ANY)
        inside = pl.BlockSpec(memory_space=pltpu.VMEM)
        args = [pltpu.with_memory_space_constraint(a, pltpu.HBM) for a in args[:8]] + [args[8]]
        outputs = (jax.ShapeDtypeStruct((2, 4), f32), vector, vector)
        found = pl.pallas_call(
            functools.partial(kernel, sizes),
            out_shape=outputs,
            in_specs=[pl.BlockSpec(memory_space=pltpu.HBM)] * 8 + [pl.BlockSpec(memory_space=pltpu.SMEM)],
            out_specs=(inside,) * 3,
            scratch_shapes=[
                pltpu.SMEM((4,), f32),
                pltpu.SMEM((4,), f32),
                pltpu.SMEM((4,), f32),
                pltpu.VMEM((6, 12, ROWS, 128), f32),
                pltpu.VMEM((10, ROWS, 128), f32),
                pltpu.VMEM((10, 8, 128), jnp.int32),
                pltpu.VMEM((3, 8, 8, 128), f32),
                pltpu.VMEM((2, 14, 8, 128), f32),
                pltpu.VMEM((2, 14, 8, 128), f32),
                pltpu.VMEM((3, 8, 128), f32),
                pltpu.VMEM((2, 2, 8, 128), f32),
                pltpu.VMEM((2, 2, 1, 8, 128), f32),
                pltpu.VMEM((2, 2, 2, 8, 128), f32),
                pltpu.VMEM((2, 2, 8, 128), f32),
                pltpu.VMEM((2, 2, 8, 128), f32),
                pltpu.VMEM((6, 6, 10, ROWS, 128), f32),
                pltpu.VMEM((sizes[2], 1, 128), f32),
                pltpu.VMEM((sizes[0] * sizes[1], 1, 128), f32),
                pltpu.SemaphoreType.DMA((8,)),
                pltpu.SemaphoreType.DMA((26,)),
                pltpu.SemaphoreType.DMA((26,)),
                pltpu.SemaphoreType.DMA((2, sizes[2])),
                pltpu.SemaphoreType.DMA((2, sizes[0] * sizes[1])),
                pltpu.SemaphoreType.REGULAR((max(1, sum(len(r) for r in known_rounds(sizes))),)),
            ],
            compiler_params=pltpu.CompilerParams(
                collective_id=0, has_side_effects=True, vmem_limit_bytes=16 * 1024 * 1024
            ),
            name="line_search",
        )(*args)
        return pl.pallas_call(
            write_out,
            out_shape=outputs,
            in_specs=[inside] * 3,
            out_specs=(anywhere,) * 3,
            scratch_shapes=[pltpu.SemaphoreType.DMA((3,))],
            compiler_params=pltpu.CompilerParams(vmem_limit_bytes=4 * 1024 * 1024),
            name="write_out",
        )(*found)

    vector, scalar = P(None, "gx", "gy", "gz"), P("gx", "gy", "gz")
    return jax.shard_map(
        body,
        mesh=mesh,
        in_specs=(vector, vector, scalar, vector, scalar, P(), P(), P(), P()),
        out_specs=(P(), vector, vector),
        check_vma=False,
    )
```

```python
import functools

import jax
import jax.numpy as jnp
from jax import lax
from jax.experimental import pallas as pl
from jax.experimental.pallas import tpu as pltpu
from jax.sharding import PartitionSpec as P

MESH = pl.DeviceIdType.MESH
LENGTHS = (1.0, 0.5, 0.25, 0.125)
ROWS = 24
TOP = 8
ALONG = ((0, 3, 4), (3, 1, 5), (4, 5, 2))


def roll(values, shift, axis):
    return pltpu.roll(values, shift % values.shape[axis], axis)


def reach(size, far):
    return sorted((k for k in range(1, size) if min(k, size - k) <= far), key=lambda k: min(k, size - k))


FAR = {"gx": 2, "gy": 2, "gz": 4}


def kernel(
    sizes,
    v_hbm, d_hbm, p_hbm, b_hbm, ph_hbm, fac_hbm, exp_hbm, yld_hbm, acc_ref,
    norms_ref, CV, CR,
    fac_ref, exp_ref, yld_ref, VP, PP, HP, BF, YS, YR, WS, ZR, XZ, YZ, ES, ER, SS, RZ, RP,
    load_sem, send_sem, recv_sem, rz_sem, rp_sem, know_sem,
):
    n = dict(zip(("gx", "gy", "gz"), sizes))
    me = {a: lax.axis_index(a) for a in n}
    has = {}
    for a in n:
        has[a, 1] = me[a] < n[a] - 1
        has[a, -1] = me[a] > 0
    f32 = jnp.float32
    lane = lax.broadcasted_iota(jnp.int32, (8, 128), 1)
    sub = lax.broadcasted_iota(jnp.int32, (8, 128), 0)
    odd = (lane & 1) == 1
    first_lane, last_lane = lane == 0, lane == 127

    block = pl.ds(TOP, 8)
    loads = [
        pltpu.make_async_copy(v_hbm, VP.at[pl.ds(0, 3), pl.ds(2, 8), block], load_sem.at[0]),
        pltpu.make_async_copy(d_hbm, VP.at[pl.ds(3, 3), pl.ds(2, 8), block], load_sem.at[1]),
        pltpu.make_async_copy(p_hbm, PP.at[pl.ds(1, 8), block], load_sem.at[2]),
        pltpu.make_async_copy(ph_hbm, HP.at[pl.ds(1, 8)], load_sem.at[3]),
        pltpu.make_async_copy(b_hbm, BF, load_sem.at[4]),
        pltpu.make_async_copy(fac_hbm, fac_ref, load_sem.at[5]),
        pltpu.make_async_copy(exp_hbm, exp_ref, load_sem.at[6]),
        pltpu.make_async_copy(yld_hbm, yld_ref, load_sem.at[7]),
    ]
    for load in loads:
        load.start()

    zero = jnp.zeros((8, 128), f32)
    for c in range(6):
        for x in (0, 1, 10, 11):
            VP[c, x, block] = zero
    for x in (0, 9):
        PP[x, block] = zero
        HP[x] = jnp.zeros((8, 128), jnp.int32)
    for ref in (YR, ZR, XZ, YZ, ER):
        ref[...] = jnp.zeros(ref.shape, f32)

    counter = [0]

    def message(step, pairs):
        send = functools.reduce(jnp.logical_and, [has[a, s] for a, s in step.items()])
        recv = functools.reduce(jnp.logical_and, [has[a, -s] for a, s in step.items()])
        target = {a: me[a] + s for a, s in step.items()}
        copies = []
        for src, dst in pairs:
            i = counter[0]
            counter[0] += 1
            copies.append(
                pltpu.make_async_remote_copy(
                    src_ref=src, dst_ref=dst, send_sem=send_sem.at[i], recv_sem=recv_sem.at[i],
                    device_id=target, device_id_type=MESH,
                )
            )
        return send, recv, copies

    def start(messages):
        for send, _, copies in messages:
            @pl.when(send)
            def _():
                for copy in copies:
                    copy.start()

    def arrived(messages):
        for _, recv, copies in messages:
            @pl.when(recv)
            def _():
                for copy in copies:
                    copy.wait_recv()

    def sent(messages):
        for send, _, copies in messages:
            @pl.when(send)
            def _():
                for copy in copies:
                    copy.wait_send()

    both = (1, -1)
    hi = lambda s: (s + 1) // 2
    lo = lambda s: (1 - s) // 2
    x_near, x_far, y_near, y_far, z_face, xz_edge, yz_edge, xy_edge = ([] for _ in range(8))
    for s in both:
        near_from, near_to = (9, 1) if s == 1 else (2, 10)
        far_from, far_to = (8, 0) if s == 1 else (3, 11)
        p_from, p_to = (8, 0) if s == 1 else (1, 9)
        x_near.append(message({"gx": s}, [
            (VP.at[:, near_from, block], VP.at[:, near_to, block]),
            (PP.at[p_from, block], PP.at[p_to, block]),
        ]))
        x_far.append(message({"gx": s}, [
            (VP.at[:, far_from, block], VP.at[:, far_to, block]),
            (HP.at[p_from], HP.at[p_to]),
        ]))
        y_near.append(message({"gy": s}, [(YS.at[hi(s), pl.ds(0, 7)], YR.at[lo(s), pl.ds(0, 7)])]))
        y_far.append(message({"gy": s}, [(YS.at[hi(s), pl.ds(7, 7)], YR.at[lo(s), pl.ds(7, 7)])]))
        z_face.append(message({"gz": s}, [(WS.at[pl.ds(0, 2)], ZR.at[lo(s)])]))
        for t in both:
            xz_edge.append(message({"gx": s, "gz": t}, [(WS.at[pl.ds(1, 1)], XZ.at[lo(s), lo(t)])]))
            yz_edge.append(message({"gy": s, "gz": t}, [(WS.at[pl.ds(1, 2)], YZ.at[lo(s), lo(t)])]))
            xy_edge.append(message({"gx": s, "gy": t}, [(ES.at[hi(s), hi(t)], ER.at[lo(s), lo(t)])]))

    barrier = pltpu.get_barrier_semaphore()

    greeted = {a: reach(n[a], FAR[a]) for a in n}

    def signal(sem, a, k):
        pl.semaphore_signal(sem, inc=1, device_id={a: lax.rem(me[a] + k, n[a])}, device_id_type=MESH)

    for a in n:
        for k in greeted[a]:
            if k in (1, n[a] - 1):
                signal(barrier, a, k)
    for a, b in (("gx", "gy"), ("gx", "gz"), ("gy", "gz")):
        for s in both:
            for t in both:
                @pl.when(jnp.logical_and(has[a, s], has[b, t]))
                def _():
                    pl.semaphore_signal(
                        barrier, inc=1, device_id={a: me[a] + s, b: me[b] + t}, device_id_type=MESH
                    )
    for a in n:
        for k in greeted[a]:
            if k not in (1, n[a] - 1):
                signal(barrier, a, k)
    sides = {a: has[a, 1].astype(jnp.int32) + has[a, -1].astype(jnp.int32) for a in n}
    edges = sides["gx"] * sides["gy"] + sides["gx"] * sides["gz"] + sides["gy"] * sides["gz"]

    ends = [(a, k) for a in ("gz", "gx") for k in greeted[a] if len(greeted[a]) < n[a] - 1 and min(k, n[a] - k) == FAR[a]]
    lines = [("gy", k) for k in greeted["gy"]]

    for load in loads[:4]:
        load.wait()

    def y_layer(c, y):
        return VP[c, pl.ds(2, 8), TOP + y]

    for side, near, far in ((0, 0, 1), (1, 7, 6)):
        for c in range(6):
            YS[side, c] = y_layer(c, near)
            YS[side, 8 + c] = y_layer(c, far)
        YS[side, 6] = PP[pl.ds(1, 8), TOP + near]
        YS[side, 7] = HP[pl.ds(1, 8), near, :].astype(f32)
        for s, xp in ((0, 2), (1, 9)):
            for c in range(6):
                ES[s, side, pl.ds(c, 1)] = VP[c, xp, pl.ds(TOP + near, 1)]

    pair = lane >> 1
    outer = jnp.where(odd, (lane + 1) >> 1, (lane >> 1) - 1) & 63
    near_z, far_z = zero, zero
    for c in range(8):
        one, two = zero, zero
        for x in range(8):
            if c < 6:
                plane = VP[c, x + 2, block]
            elif c == 6:
                plane = PP[x + 1, block]
            else:
                plane = HP[x + 1].astype(f32)
            k = 8 * c + x
            turned = roll(plane, 2 * k + 1, 1)
            one = jnp.where(pair == k, turned, one)
            if c < 6:
                two = jnp.where(outer == k, turned, two)
        near_z = jnp.where((lane >> 4) == c, one, near_z)
        if c < 6:
            far_z = jnp.where((outer >> 3) == c, two, far_z)
    WS[0] = far_z
    WS[1] = near_z
    near_zy = zero
    for side in range(2):
        for c in range(6):
            k = 8 * side + c
            near_zy = jnp.where(pair == k, roll(YS[side, c], 2 * k + 1, 1), near_zy)
    WS[2] = near_zy

    pl.semaphore_wait(barrier, sum(len(ks) for ks in greeted.values()) + edges)
    for group in (x_near, y_near, z_face, xy_edge, xz_edge, yz_edge, x_far, y_far):
        start(group)
    for a, k in ends:
        signal(know_sem.at[0], a, k)

    for load in loads[5:]:
        load.wait()
    picked = acc_ref[0]
    length = jnp.where(
        picked == 0, f32(1.0), jnp.where(picked == 1, f32(0.5), jnp.where(picked == 2, f32(0.25), f32(0.125)))
    )
    for c in range(3):
        for x in range(8):
            CV[c, x] = VP[c, x + 2, block] + length * VP[3 + c, x + 2, block]

    full = lambda s: jnp.full((8, 128), s, f32)
    table = []
    for k in range(4):
        exponent = full(exp_ref[k])
        table.append((full(fac_ref[k]), (1.0 - exponent) / (2.0 * exponent), full(0.5 * yld_ref[k])))

    def params(ids):
        out = table[3]
        for k in (2, 1, 0):
            hit = ids == k
            out = tuple(jnp.where(hit, mine, other) for mine, other in zip(table[k], out))
        return out

    def tensor(g):
        return (
            g[0][0], g[1][1], g[2][2],
            0.5 * (g[0][1] + g[1][0]), 0.5 * (g[0][2] + g[2][0]), 0.5 * (g[1][2] + g[2][1]),
        )

    def dot(a, b):
        return (a[0] * b[0] + a[1] * b[1] + a[2] * b[2]) + 2.0 * (a[3] * b[3] + a[4] * b[4] + a[5] * b[5])

    def flow(second, factor, power, half_yield):
        inverse = lax.rsqrt(second)
        creep = factor * jnp.exp(power * jnp.log(second))
        plastic = half_yield * inverse
        total = creep + plastic
        return inverse, creep, plastic, total, creep * plastic / total

    def stresses(g, ids, wanted, mask=None):
        factor, power, half_yield = params(ids)
        base, change = tensor(g[:3]), tensor(g[3:])
        inverse, creep, plastic, total, harmonic = flow(0.125 * dot(base, base) + 0.01, factor, power, half_yield)
        viscosity = harmonic + 0.05
        slope = harmonic * (inverse * inverse) * (plastic * power - 0.5 * creep) / total
        along = slope * (0.25 * dot(base, change))
        if mask is not None:
            viscosity, along = viscosity * mask, along * mask
        fields = [
            {c: viscosity * base[c] for c in wanted},
            {c: viscosity * change[c] + along * base[c] for c in wanted},
        ]
        for a in LENGTHS:
            trial = tuple(e + f if a == 1.0 else e + a * f for e, f in zip(base, change))
            viscosity = flow(0.125 * dot(trial, trial) + 0.01, factor, power, half_yield)[4] + 0.05
            if mask is not None:
                viscosity = viscosity * mask
            fields.append({c: viscosity * trial[c] for c in wanted})
        return fields

    def across_z(plane, ends):
        return jnp.where(last_lane, ends, roll(plane, -1, 1)) - jnp.where(first_lane, ends, roll(plane, 1, 1))

    def ends_of(packed, k):
        return roll(packed, -(2 * k + 1), 1)

    def joined(below, above):
        return jnp.where(odd, roll(below, 1, 1), roll(above, -1, 1))

    def flag(a, s):
        return has[a, s].astype(f32)

    def plane_differences(xp, packed, x):
        g = []
        for c in range(6):
            centre = VP[c, xp, block]
            g.append((
                VP[c, xp + 1, block] - VP[c, xp - 1, block],
                VP[c, xp, pl.ds(TOP + 1, 8)] - VP[c, xp, pl.ds(TOP - 1, 8)],
                across_z(centre, ends_of(packed, 8 * c + x)),
            ))
        return g

    every = tuple(range(6))

    def store_plane(xs, fields):
        for f, field in enumerate(fields):
            for c, value in field.items():
                SS[f, c, xs, block] = value

    arrived(z_face)
    arrived(y_near)
    near_halo = joined(ZR[0, 1], ZR[1, 1])
    far_halo = jnp.where(odd, roll(ZR[0, 0], 2, 1), roll(ZR[1, 0], -2, 1))
    for side, row in ((0, TOP - 1), (1, TOP + 8)):
        for c in range(6):
            VP[c, pl.ds(2, 8), row] = YR[side, c]
        PP[pl.ds(1, 8), row] = YR[side, 6]
    for x in range(1, 7):
        store_plane(x + 1, stresses(plane_differences(x + 2, near_halo, x), HP[x + 1], every))

    arrived(x_near)
    for x in (0, 7):
        store_plane(x + 1, stresses(plane_differences(x + 2, near_halo, x), HP[x + 1], every))
    arrived(xy_edge)
    arrived(xz_edge)
    x_ends = [joined(XZ[side, 0, 0], XZ[side, 1, 0]) for side in range(2)]
    for s, xp in ((0, 1), (1, 10)):
        for t, row in ((0, TOP - 1), (1, TOP + 8)):
            for c in range(6):
                VP[c, xp, pl.ds(row, 1)] = ER[s, t, pl.ds(c, 1)]
    arrived(x_far)
    for side, xp, x in ((0, 1, 7), (1, 10, 0)):
        g = plane_differences(xp, x_ends[side], x)
        store_plane(xp - 1, stresses(g, HP[xp - 1], ALONG[0], flag("gx", 2 * side - 1)))

    arrived(yz_edge)
    arrived(y_far)
    for side in range(2):
        packed = joined(YZ[side, 0, 1], YZ[side, 1, 1])
        g = []
        for c in range(6):
            centre = YR[side, c]
            above = jnp.where(sub == 7, ER[1, side, pl.ds(c, 1)], roll(centre, -1, 0))
            below = jnp.where(sub == 0, ER[0, side, pl.ds(c, 1)], roll(centre, 1, 0))
            outward = YS[side, c] - YR[side, 8 + c]
            g.append((
                above - below,
                outward if side == 0 else -outward,
                across_z(centre, ends_of(packed, 8 * (1 - side) + c)),
            ))
        fields = stresses(g, YR[side, 7], ALONG[1], flag("gy", 2 * side - 1))
        row = TOP - 1 if side == 0 else TOP + 8
        for f, field in enumerate(fields):
            for c, value in field.items():
                SS[f, c, pl.ds(1, 8), row] = value

    inner = WS[1]
    y_ends = [joined(YZ[side, 0, 0], YZ[side, 1, 0]) for side in range(2)]
    column = pair & 7
    out_z = jnp.where(odd, inner - far_halo, far_halo - inner)
    out_y = roll(jnp.where(sub == 0, y_ends[1], near_halo), -1, 0) - roll(
        jnp.where(sub == 7, y_ends[0], near_halo), 1, 0
    )
    out_x = jnp.where(column == 7, roll(x_ends[1], 14, 1), roll(near_halo, -2, 1)) - jnp.where(
        column == 0, roll(x_ends[0], -14, 1), roll(near_halo, 2, 1)
    )
    g = [tuple(roll(o, -16 * c, 1) if c else o for o in (out_x, out_y, out_z)) for c in range(6)]
    mask = jnp.where(odd, flag("gz", -1), flag("gz", 1))
    z_fields = stresses(g, roll(near_halo, -112, 1), ALONG[2], mask)

    if ends:
        pl.semaphore_wait(know_sem.at[0], len(ends))
    for a, k in lines:
        signal(know_sem.at[1], a, k)

    loads[4].wait()
    sums = [zero] * 8
    for x in range(8):
        xs = x + 1
        p_plane = PP[xs, block]
        slope = (
            PP[xs + 1, block] - PP[xs - 1, block],
            PP[xs, pl.ds(TOP + 1, 8)] - PP[xs, pl.ds(TOP - 1, 8)],
            across_z(p_plane, ends_of(near_halo, 48 + x)),
        )
        for i in range(3):
            loading = BF[i, x] - 0.5 * slope[i]
            cx, cy, cz = ALONG[0][i], ALONG[1][i], ALONG[2][i]
            out = []
            for f in range(6):
                change = SS[f, cx, xs + 1, block] - SS[f, cx, xs - 1, block]
                change = change + (SS[f, cy, xs, pl.ds(TOP + 1, 8)] - SS[f, cy, xs, pl.ds(TOP - 1, 8)])
                change = change + across_z(SS[f, cz, xs, block], ends_of(z_fields[f][cz], x))
                out.append(0.5 * change if f == 1 else 0.5 * change + loading)
            chosen = out[5]
            for k in (2, 1, 0):
                chosen = jnp.where(picked == k, out[2 + k], chosen)
            CR[i, x] = chosen
            for k, a in enumerate(LENGTHS):
                sums[k] = sums[k] + out[2 + k] * out[2 + k]
                linear = out[0] + a * out[1]
                sums[4 + k] = sums[4 + k] + linear * linear

    stacked = zero
    for k in range(8):
        stacked = jnp.where(sub == k, jnp.sum(sums[k], axis=0, keepdims=True), stacked)
    totals = jnp.sum(stacked, axis=1, keepdims=True)
    row = jnp.sum(jnp.where(lane == sub, totals, 0.0), axis=0, keepdims=True)
    shares = []
    for axes, ref, sems in ((("gz",), RZ, rz_sem), (("gx", "gy"), RP, rp_sem)):
        offsets = [()]
        for a in axes:
            offsets = [o + (k,) for o in offsets for k in range(n[a])]
        hops = lambda o: sum(min(k, n[a] - k) for k, a in zip(o, axes))
        mine = 0
        for a in axes:
            mine = mine * n[a] + me[a]
        ref[mine] = row
        if len(axes) == 2:
            pl.semaphore_wait(know_sem.at[1], len(lines))
        copies = []
        for i, o in sorted(enumerate(offsets), key=lambda item: -hops(item[1])):
            if any(o):
                copies.append(
                    pltpu.make_async_remote_copy(
                        src_ref=ref.at[mine], dst_ref=ref.at[mine],
                        send_sem=sems.at[0, i], recv_sem=sems.at[1, i],
                        device_id={a: lax.rem(me[a] + k, n[a]) for k, a in zip(o, axes)},
                        device_id_type=MESH,
                    )
                )
        for copy in copies:
            copy.start()
        for copy in copies:
            copy.wait_recv()
        rows = [ref[k] for k in range(len(offsets))]
        while len(rows) > 1:
            rows = [sum(rows[k:k + 2]) for k in range(0, len(rows), 2)]
        row = rows[0]
        shares += copies
    cells = 3.0 * (8 * n["gx"]) * (8 * n["gy"]) * (128 * n["gz"])
    norms = jnp.sqrt(row / cells + 1e-6)
    norms_ref[pl.ds(0, 1)] = norms[:, 0:4]
    norms_ref[pl.ds(1, 1)] = roll(jnp.broadcast_to(norms, (8, 128)), -4, 1)[0:1, 0:4]

    for copy in shares:
        copy.wait_send()
    for group in (x_near, y_near, z_face, xy_edge, xz_edge, yz_edge, x_far, y_far):
        sent(group)


def write_out(*refs):
    copies = [pltpu.make_async_copy(refs[i], refs[3 + i], refs[6].at[i]) for i in range(3)]
    for copy in copies:
        copy.start()
    for copy in copies:
        copy.wait()


def solution(mesh):
    sizes = tuple(mesh.shape[a] for a in ("gx", "gy", "gz"))
    f32 = jnp.float32

    def body(*args):
        vector = jax.ShapeDtypeStruct((3, 8, 8, 128), f32)
        anywhere = pl.BlockSpec(memory_space=pl.ANY)
        inside = pl.BlockSpec(memory_space=pltpu.VMEM)
        args = [pltpu.with_memory_space_constraint(a, pltpu.HBM) for a in args[:8]] + [args[8]]
        outputs = (jax.ShapeDtypeStruct((2, 4), f32), vector, vector)
        found = pl.pallas_call(
            functools.partial(kernel, sizes),
            out_shape=outputs,
            in_specs=[pl.BlockSpec(memory_space=pltpu.HBM)] * 8 + [pl.BlockSpec(memory_space=pltpu.SMEM)],
            out_specs=(inside,) * 3,
            scratch_shapes=[
                pltpu.SMEM((4,), f32),
                pltpu.SMEM((4,), f32),
                pltpu.SMEM((4,), f32),
                pltpu.VMEM((6, 12, ROWS, 128), f32),
                pltpu.VMEM((10, ROWS, 128), f32),
                pltpu.VMEM((10, 8, 128), jnp.int32),
                pltpu.VMEM((3, 8, 8, 128), f32),
                pltpu.VMEM((2, 14, 8, 128), f32),
                pltpu.VMEM((2, 14, 8, 128), f32),
                pltpu.VMEM((3, 8, 128), f32),
                pltpu.VMEM((2, 2, 8, 128), f32),
                pltpu.VMEM((2, 2, 1, 8, 128), f32),
                pltpu.VMEM((2, 2, 2, 8, 128), f32),
                pltpu.VMEM((2, 2, 8, 128), f32),
                pltpu.VMEM((2, 2, 8, 128), f32),
                pltpu.VMEM((6, 6, 10, ROWS, 128), f32),
                pltpu.VMEM((sizes[2], 1, 128), f32),
                pltpu.VMEM((sizes[0] * sizes[1], 1, 128), f32),
                pltpu.SemaphoreType.DMA((8,)),
                pltpu.SemaphoreType.DMA((26,)),
                pltpu.SemaphoreType.DMA((26,)),
                pltpu.SemaphoreType.DMA((2, sizes[2])),
                pltpu.SemaphoreType.DMA((2, sizes[0] * sizes[1])),
                pltpu.SemaphoreType.REGULAR((2,)),
            ],
            compiler_params=pltpu.CompilerParams(
                collective_id=0, has_side_effects=True, vmem_limit_bytes=16 * 1024 * 1024
            ),
            name="line_search",
        )(*args)
        return pl.pallas_call(
            write_out,
            out_shape=outputs,
            in_specs=[inside] * 3,
            out_specs=(anywhere,) * 3,
            scratch_shapes=[pltpu.SemaphoreType.DMA((3,))],
            compiler_params=pltpu.CompilerParams(vmem_limit_bytes=4 * 1024 * 1024),
            name="write_out",
        )(*found)

    vector, scalar = P(None, "gx", "gy", "gz"), P("gx", "gy", "gz")
    return jax.shard_map(
        body,
        mesh=mesh,
        in_specs=(vector, vector, scalar, vector, scalar, P(), P(), P(), P()),
        out_specs=(P(), vector, vector),
        check_vma=False,
    )
```

```python
import functools

import jax
import jax.numpy as jnp
from jax import lax
from jax.experimental import pallas as pl
from jax.experimental.pallas import tpu as pltpu
from jax.sharding import PartitionSpec as P

MESH = pl.DeviceIdType.MESH
LENGTHS = (1.0, 0.5, 0.25, 0.125)
ROWS = 24
TOP = 8
TOGETHER = 6
ALONG = ((0, 3, 4), (3, 1, 5), (4, 5, 2))


def roll(values, shift, axis):
    return pltpu.roll(values, shift % values.shape[axis], axis)


def reach(size, far):
    return sorted((k for k in range(1, size) if min(k, size - k) <= far), key=lambda k: min(k, size - k))


def doubling(step, end):
    found = []
    while step < end:
        found.append(step)
        step *= 2
    return found


def take_rows(ref, start, row):
    return ref.reshape(ref.shape[0] * ROWS, 128)[pl.ds(start * ROWS + row, 8, stride=ROWS), :]


def put_rows(ref, start, row, value):
    ref.reshape(ref.shape[0] * ROWS, 128)[pl.ds(start * ROWS + row, 8, stride=ROWS), :] = value


def kernel(
    sizes,
    v_hbm, d_hbm, p_hbm, b_hbm, ph_hbm, fac_hbm, exp_hbm, yld_hbm, acc_ref,
    norms_ref, CV, CR,
    fac_ref, exp_ref, yld_ref, VP, PP, HP, BF, YS, YR, WS, ZR, XZ, YZ, ES, ER, SS, PR, RZ, RP,
    load_sem, send_sem, recv_sem, sum_sem, know_sem,
):
    n = dict(zip(("gx", "gy", "gz"), sizes))
    me = {a: lax.axis_index(a) for a in n}
    has = {}
    for a in n:
        has[a, 1] = me[a] < n[a] - 1
        has[a, -1] = me[a] > 0
    f32 = jnp.float32
    lane = lax.broadcasted_iota(jnp.int32, (8, 128), 1)
    sub = lax.broadcasted_iota(jnp.int32, (8, 128), 0)
    odd = (lane & 1) == 1
    first_lane, last_lane = lane == 0, lane == 127

    block = pl.ds(TOP, 8)
    loads = [
        pltpu.make_async_copy(v_hbm, VP.at[pl.ds(0, 3), pl.ds(2, 8), block], send_sem.at[0]),
        pltpu.make_async_copy(d_hbm, VP.at[pl.ds(3, 3), pl.ds(2, 8), block], send_sem.at[1]),
        pltpu.make_async_copy(p_hbm, PP.at[pl.ds(1, 8), block], send_sem.at[2]),
        pltpu.make_async_copy(ph_hbm, HP.at[pl.ds(1, 8)], send_sem.at[3]),
        pltpu.make_async_copy(b_hbm, BF, load_sem.at[0]),
        pltpu.make_async_copy(fac_hbm, fac_ref, load_sem.at[1]),
        pltpu.make_async_copy(exp_hbm, exp_ref, load_sem.at[2]),
        pltpu.make_async_copy(yld_hbm, yld_ref, load_sem.at[3]),
    ]
    for load in loads:
        load.start()

    zero = jnp.zeros((8, 128), f32)
    for c in range(6):
        for x in (0, 1, 10, 11):
            VP[c, x, block] = zero
    for x in (0, 9):
        PP[x, block] = zero
        HP[x] = jnp.zeros((8, 128), jnp.int32)
    for ref in (YR, ZR, XZ, YZ, ER):
        ref[...] = jnp.zeros(ref.shape, f32)

    senders, counter = {}, [0]

    def remote(src, dst, i, j, target):
        return pltpu.make_async_remote_copy(
            src_ref=src, dst_ref=dst, send_sem=send_sem.at[i], recv_sem=recv_sem.at[j],
            device_id=target, device_id_type=MESH,
        )

    def message(step, pairs, whole=None):
        send = functools.reduce(jnp.logical_and, [has[a, s] for a, s in step.items()])
        recv = functools.reduce(jnp.logical_and, [has[a, -s] for a, s in step.items()])
        target = {a: me[a] + s for a, s in step.items()}
        i = senders.setdefault(tuple(step.items()), len(senders))
        j = counter[0]
        counter[0] += 1
        copies = [remote(src, dst, i, j, target) for src, dst in pairs]
        return send, recv, copies, remote(whole, whole, i, j, target) if whole is not None else copies[0]

    def start(messages):
        for send, _, copies, _ in messages:
            @pl.when(send)
            def _():
                for copy in copies:
                    copy.start()

    def arrived(messages):
        for _, recv, _, wait in messages:
            @pl.when(recv)
            def _():
                wait.wait_recv()

    def sent():
        for step, i in senders.items():
            size = {1: YS.at[0] if step[0][0] != "gz" else WS.at[pl.ds(0, 2)]}.get(len(step))
            if size is None:
                names = {step[0][0], step[1][0]}
                size = WS.at[pl.ds(0, 2)] if names == {"gy", "gz"} else WS.at[pl.ds(0, 1)]
            send = functools.reduce(jnp.logical_and, [has[a, s] for a, s in step])

            @pl.when(send)
            def _():
                remote(size, size, i, 0, {a: me[a] + s for a, s in step}).wait_send()

    both = (1, -1)
    hi = lambda s: (s + 1) // 2
    lo = lambda s: (1 - s) // 2
    x_near, x_far, y_near, y_far, z_face, xz_edge, yz_edge, xy_edge = ([] for _ in range(8))
    for s in both:
        near_from, near_to = (9, 1) if s == 1 else (2, 10)
        far_from, far_to = (8, 0) if s == 1 else (3, 11)
        p_from, p_to = (8, 0) if s == 1 else (1, 9)
        x_near.append(message({"gx": s}, [
            (VP.at[:, near_from, block], VP.at[:, near_to, block]),
            (PP.at[p_from, block], PP.at[p_to, block]),
        ], YR.at[lo(s), pl.ds(0, 7)]))
        x_far.append(message({"gx": s}, [
            (VP.at[:, far_from, block], VP.at[:, far_to, block]),
            (HP.at[p_from], HP.at[p_to]),
        ], YR.at[lo(s), pl.ds(7, 7)]))
        y_near.append(message({"gy": s}, [(YS.at[hi(s), pl.ds(0, 7)], YR.at[lo(s), pl.ds(0, 7)])]))
        y_far.append(message({"gy": s}, [(YS.at[hi(s), pl.ds(7, 7)], YR.at[lo(s), pl.ds(7, 7)])]))
        z_face.append(message({"gz": s}, [(WS.at[pl.ds(0, 2)], ZR.at[lo(s)])]))
        for t in both:
            xz_edge.append(message({"gx": s, "gz": t}, [(WS.at[pl.ds(1, 1)], XZ.at[lo(s), lo(t)])]))
            yz_edge.append(message({"gy": s, "gz": t}, [(WS.at[pl.ds(1, 2)], YZ.at[lo(s), lo(t)])]))
            xy_edge.append(message({"gx": s, "gy": t}, [(ES.at[hi(s), hi(t)], ER.at[lo(s), lo(t)])]))

    barrier = pltpu.get_barrier_semaphore()

    greeted = {"gz": reach(n["gz"], 2), "gy": reach(n["gy"], 2)}

    def signal(sem, a, k):
        pl.semaphore_signal(sem, inc=1, device_id={a: lax.rem(me[a] + k, n[a])}, device_id_type=MESH)

    def signal_x(sem, step):
        for s in (step, -step):
            there = jnp.logical_and(me["gx"] + s >= 0, me["gx"] + s < n["gx"])

            @pl.when(there)
            def _():
                pl.semaphore_signal(sem, inc=1, device_id={"gx": me["gx"] + s}, device_id_type=MESH)

    def count_x(step):
        return (me["gx"] + step < n["gx"]).astype(jnp.int32) + (me["gx"] - step >= 0).astype(jnp.int32)

    for a, b in (("gx", "gy"), ("gx", "gz"), ("gy", "gz")):
        for s in both:
            for t in both:
                @pl.when(jnp.logical_and(has[a, s], has[b, t]))
                def _():
                    pl.semaphore_signal(
                        barrier, inc=1, device_id={a: me[a] + s, b: me[b] + t}, device_id_type=MESH
                    )
    for a in greeted:
        for k in greeted[a]:
            signal(barrier, a, k)
    signal_x(barrier, 1)
    sides = {a: has[a, 1].astype(jnp.int32) + has[a, -1].astype(jnp.int32) for a in n}
    edges = sides["gx"] * sides["gy"] + sides["gx"] * sides["gz"] + sides["gy"] * sides["gz"]

    z_rounds = doubling(2, n["gz"] // 2)
    x_rounds = doubling(1, n["gx"])

    def tell_z(r):
        if r < len(z_rounds):
            for k in (z_rounds[r], n["gz"] - z_rounds[r]):
                signal(know_sem.at[0, r], "gz", k)

    def told_z(r):
        if r < len(z_rounds):
            pl.semaphore_wait(know_sem.at[0, r], 2)

    def tell_x(r):
        if r < len(x_rounds):
            signal_x(know_sem.at[1, r], x_rounds[r])

    def told_x(r):
        if r < len(x_rounds):
            pl.semaphore_wait(know_sem.at[1, r], count_x(x_rounds[r]))

    for load in loads[:4]:
        load.wait()

    def y_layer(c, y):
        return take_rows(VP.at[c], 2, TOP + y)

    for side, near, far in ((0, 0, 1), (1, 7, 6)):
        for c in range(6):
            YS[side, c] = y_layer(c, near)
            YS[side, 8 + c] = y_layer(c, far)
        YS[side, 6] = take_rows(PP, 1, TOP + near)
        YS[side, 7] = HP[pl.ds(1, 8), near, :].astype(f32)
        for s, xp in ((0, 2), (1, 9)):
            for c in range(6):
                ES[s, side, pl.ds(c, 1)] = VP[c, xp, pl.ds(TOP + near, 1)]

    pair = lane >> 1
    outer = jnp.where(odd, (lane + 1) >> 1, (lane >> 1) - 1) & 63
    near_z, far_z = zero, zero
    for c in range(8):
        one, two = zero, zero
        for x in range(8):
            if c < 6:
                plane = VP[c, x + 2, block]
            elif c == 6:
                plane = PP[x + 1, block]
            else:
                plane = HP[x + 1].astype(f32)
            k = 8 * c + x
            turned = roll(plane, 2 * k + 1, 1)
            one = jnp.where(pair == k, turned, one)
            if c < 6:
                two = jnp.where(outer == k, turned, two)
        near_z = jnp.where((lane >> 4) == c, one, near_z)
        if c < 6:
            far_z = jnp.where((outer >> 3) == c, two, far_z)
    WS[0] = far_z
    WS[1] = near_z
    near_zy = zero
    for side in range(2):
        for c in range(6):
            k = 8 * side + c
            near_zy = jnp.where(pair == k, roll(YS[side, c], 2 * k + 1, 1), near_zy)
    WS[2] = near_zy

    pl.semaphore_wait(barrier, sum(len(ks) for ks in greeted.values()) + sides["gx"] + edges)
    for group in (z_face, x_near, xz_edge, y_near, xy_edge, yz_edge, x_far, y_far):
        start(group)
    tell_z(0)
    tell_x(0)

    for load in loads[5:]:
        load.wait()
    picked = acc_ref[0]
    length = jnp.where(
        picked == 0, f32(1.0), jnp.where(picked == 1, f32(0.5), jnp.where(picked == 2, f32(0.25), f32(0.125)))
    )
    for c in range(3):
        for x in range(8):
            CV[c, x] = VP[c, x + 2, block] + length * VP[3 + c, x + 2, block]

    full = lambda s: jnp.full((8, 128), s, f32)
    table = []
    for k in range(4):
        exponent = full(exp_ref[k])
        table.append((full(fac_ref[k]), (1.0 - exponent) / (2.0 * exponent), full(0.5 * yld_ref[k])))

    def params(ids):
        out = table[3]
        for k in (2, 1, 0):
            hit = ids == k
            out = tuple(jnp.where(hit, mine, other) for mine, other in zip(table[k], out))
        return out

    for x in range(8):
        for i, value in enumerate(params(HP[x + 1])):
            PR[i, x] = value

    def tensor(g):
        return (
            g[0][0], g[1][1], g[2][2],
            0.5 * (g[0][1] + g[1][0]), 0.5 * (g[0][2] + g[2][0]), 0.5 * (g[1][2] + g[2][1]),
        )

    def dot(a, b):
        return (a[0] * b[0] + a[1] * b[1] + a[2] * b[2]) + 2.0 * (a[3] * b[3] + a[4] * b[4] + a[5] * b[5])

    def flow(second, factor, power, half_yield):
        inverse = lax.rsqrt(second)
        creep = factor * jnp.exp(power * jnp.log(second))
        plastic = half_yield * inverse
        total = creep + plastic
        return inverse, creep, plastic, total, creep * plastic / total

    def stresses(g, material, wanted, mask=None):
        factor, power, half_yield = material
        base, change = tensor(g[:3]), tensor(g[3:])
        inverse, creep, plastic, total, harmonic = flow(0.125 * dot(base, base) + 0.01, factor, power, half_yield)
        viscosity = 0.5 * harmonic + 0.025
        slope = harmonic * (inverse * inverse) * (plastic * power - 0.5 * creep) / total
        along = slope * (0.125 * dot(base, change))
        if mask is not None:
            viscosity, along = viscosity * mask, along * mask
        fields = [
            {c: viscosity * base[c] for c in wanted},
            {c: viscosity * change[c] + along * base[c] for c in wanted},
        ]
        for a in LENGTHS:
            trial = tuple(e + f if a == 1.0 else e + a * f for e, f in zip(base, change))
            viscosity = 0.5 * flow(0.125 * dot(trial, trial) + 0.01, factor, power, half_yield)[4] + 0.025
            if mask is not None:
                viscosity = viscosity * mask
            fields.append({c: viscosity * trial[c] for c in wanted})
        return fields

    def across_z(plane, ends):
        return jnp.where(last_lane, ends, roll(plane, -1, 1)) - jnp.where(first_lane, ends, roll(plane, 1, 1))

    def ends_of(packed, k):
        return pltpu.roll(packed, 127 - 2 * k, 1)

    def joined(below, above):
        return jnp.where(odd, roll(below, 1, 1), roll(above, -1, 1))

    def flag(a, s):
        return has[a, s].astype(f32)

    def plane_differences(xp, packed, x):
        g = []
        for c in range(6):
            centre = VP[c, xp, block]
            g.append((
                VP[c, xp + 1, block] - VP[c, xp - 1, block],
                VP[c, xp, pl.ds(TOP + 1, 8)] - VP[c, xp, pl.ds(TOP - 1, 8)],
                across_z(centre, ends_of(packed, 8 * c + x)),
            ))
        return g

    every = tuple(range(6))

    def store_plane(xs, fields):
        for f, field in enumerate(fields):
            for c, value in field.items():
                SS[f, c, xs, block] = value

    told_z(0)
    tell_z(1)
    told_x(0)
    tell_x(1)
    arrived(z_face)
    arrived(y_near)
    near_halo = joined(ZR[0, 1], ZR[1, 1])
    far_halo = jnp.where(odd, roll(ZR[0, 0], 2, 1), roll(ZR[1, 0], -2, 1))
    for side, row in ((0, TOP - 1), (1, TOP + 8)):
        for c in range(6):
            put_rows(VP.at[c], 2, row, YR[side, c])
        put_rows(PP, 1, row, YR[side, 6])

    def own_plane(x):
        material = tuple(PR[i, x] for i in range(3))
        store_plane(x + 1, stresses(plane_differences(x + 2, near_halo, x), material, every))

    def some_planes(i, carry):
        for k in range(TOGETHER):
            own_plane(1 + TOGETHER * i + k)
        return carry

    lax.fori_loop(0, 6 // TOGETHER, some_planes, 0)

    arrived(x_near)
    own_plane(0)
    own_plane(7)
    arrived(xz_edge)
    arrived(yz_edge)
    x_ends = [joined(XZ[side, 0, 0], XZ[side, 1, 0]) for side in range(2)]
    inner = WS[1]
    y_ends = [joined(YZ[side, 0, 0], YZ[side, 1, 0]) for side in range(2)]
    column = pair & 7
    out_z = jnp.where(odd, inner - far_halo, far_halo - inner)
    out_y = roll(jnp.where(sub == 0, y_ends[1], near_halo), -1, 0) - roll(
        jnp.where(sub == 7, y_ends[0], near_halo), 1, 0
    )
    out_x = jnp.where(column == 7, roll(x_ends[1], 14, 1), roll(near_halo, -2, 1)) - jnp.where(
        column == 0, roll(x_ends[0], -14, 1), roll(near_halo, 2, 1)
    )
    g = [tuple(roll(o, -16 * c, 1) if c else o for o in (out_x, out_y, out_z)) for c in range(6)]
    mask = jnp.where(odd, flag("gz", -1), flag("gz", 1))
    z_fields = stresses(g, params(roll(near_halo, -112, 1)), ALONG[2], mask)

    arrived(xy_edge)
    arrived(y_far)
    for side in range(2):
        packed = joined(YZ[side, 0, 1], YZ[side, 1, 1])
        g = []
        for c in range(6):
            centre = YR[side, c]
            above = jnp.where(sub == 7, ER[1, side, pl.ds(c, 1)], roll(centre, -1, 0))
            below = jnp.where(sub == 0, ER[0, side, pl.ds(c, 1)], roll(centre, 1, 0))
            outward = YS[side, c] - YR[side, 8 + c]
            g.append((
                above - below,
                outward if side == 0 else -outward,
                across_z(centre, ends_of(packed, 8 * (1 - side) + c)),
            ))
        fields = stresses(g, params(YR[side, 7]), ALONG[1], flag("gy", 2 * side - 1))
        row = TOP - 1 if side == 0 else TOP + 8
        for f, field in enumerate(fields):
            for c, value in field.items():
                put_rows(SS.at[f, c], 1, row, value)

    for s, xp in ((0, 1), (1, 10)):
        for t, row in ((0, TOP - 1), (1, TOP + 8)):
            for c in range(6):
                VP[c, xp, pl.ds(row, 1)] = ER[s, t, pl.ds(c, 1)]
    arrived(x_far)
    for side, xp, x in ((0, 1, 7), (1, 10, 0)):
        g = plane_differences(xp, x_ends[side], x)
        store_plane(xp - 1, stresses(g, params(HP[xp - 1]), ALONG[0], flag("gx", 2 * side - 1)))

    for r in range(1, len(z_rounds)):
        told_z(r)
        tell_z(r + 1)
    told_x(1)
    tell_x(2)

    loads[4].wait()
    sums = [zero] * 8
    for x in range(8):
        xs = x + 1
        p_plane = PP[xs, block]
        slope = (
            PP[xs + 1, block] - PP[xs - 1, block],
            PP[xs, pl.ds(TOP + 1, 8)] - PP[xs, pl.ds(TOP - 1, 8)],
            across_z(p_plane, ends_of(near_halo, 48 + x)),
        )
        for i in range(3):
            loading = BF[i, x] - 0.5 * slope[i]
            cx, cy, cz = ALONG[0][i], ALONG[1][i], ALONG[2][i]
            out = []
            for f in range(6):
                change = SS[f, cx, xs + 1, block] - SS[f, cx, xs - 1, block]
                change = change + (SS[f, cy, xs, pl.ds(TOP + 1, 8)] - SS[f, cy, xs, pl.ds(TOP - 1, 8)])
                change = change + across_z(SS[f, cz, xs, block], ends_of(z_fields[f][cz], x))
                out.append(change if f == 1 else change + loading)
            chosen = out[5]
            for k in (2, 1, 0):
                chosen = jnp.where(picked == k, out[2 + k], chosen)
            CR[i, x] = chosen
            for k, a in enumerate(LENGTHS):
                sums[k] = sums[k] + out[2 + k] * out[2 + k]
                linear = out[0] + a * out[1]
                sums[4 + k] = sums[4 + k] + linear * linear

    stacked = zero
    for k in range(8):
        stacked = jnp.where(sub == k, jnp.sum(sums[k], axis=0, keepdims=True), stacked)
    totals = jnp.sum(stacked, axis=1, keepdims=True)
    row = jnp.sum(jnp.where(lane == sub, totals, 0.0), axis=0, keepdims=True)
    for stage, (axes, ref) in enumerate(((("gz",), RZ), (("gx", "gy"), RP))):
        offsets = [()]
        for a in axes:
            offsets = [o + (k,) for o in offsets for k in range(n[a])]
        hops = lambda o: sum(min(k, n[a] - k) for k, a in zip(o, axes))
        mine = 0
        for a in axes:
            mine = mine * n[a] + me[a]
        if len(axes) == 2:
            for r in range(2, len(x_rounds)):
                told_x(r)
                tell_x(r + 1)
        ref[mine] = row

        def share(rows, target):
            return pltpu.make_async_remote_copy(
                src_ref=rows, dst_ref=rows, send_sem=load_sem.at[stage], recv_sem=sum_sem.at[stage],
                device_id=target, device_id_type=MESH,
            )

        others = sorted((o for o in offsets if any(o)), key=lambda o: -hops(o))
        targets = [{a: lax.rem(me[a] + k, n[a]) for k, a in zip(o, axes)} for o in others]
        for target in targets:
            share(ref.at[mine], target).start()
        if stage == 0:
            sent()
        whole = share(ref.at[pl.ds(0, len(others))], targets[0])
        whole.wait_send()
        whole.wait_recv()
        rows = [ref[k] for k in range(len(offsets))]
        while len(rows) > 1:
            rows = [sum(rows[k:k + 2]) for k in range(0, len(rows), 2)]
        row = rows[0]
    cells = 3.0 * (8 * n["gx"]) * (8 * n["gy"]) * (128 * n["gz"])
    norms = jnp.sqrt(row / cells + 1e-6)
    norms_ref[pl.ds(0, 1)] = norms[:, 0:4]
    norms_ref[pl.ds(1, 1)] = roll(jnp.broadcast_to(norms, (8, 128)), -4, 1)[0:1, 0:4]


def write_out(*refs):
    copies = [pltpu.make_async_copy(refs[i], refs[3 + i], refs[6].at[i]) for i in range(3)]
    for copy in copies:
        copy.start()
    for copy in copies:
        copy.wait()


def solution(mesh):
    sizes = tuple(mesh.shape[a] for a in ("gx", "gy", "gz"))
    f32 = jnp.float32

    def body(*args):
        vector = jax.ShapeDtypeStruct((3, 8, 8, 128), f32)
        anywhere = pl.BlockSpec(memory_space=pl.ANY)
        inside = pl.BlockSpec(memory_space=pltpu.VMEM)
        args = [pltpu.with_memory_space_constraint(a, pltpu.HBM) for a in args[:8]] + [args[8]]
        outputs = (jax.ShapeDtypeStruct((2, 4), f32), vector, vector)
        found = pl.pallas_call(
            functools.partial(kernel, sizes),
            out_shape=outputs,
            in_specs=[pl.BlockSpec(memory_space=pltpu.HBM)] * 8 + [pl.BlockSpec(memory_space=pltpu.SMEM)],
            out_specs=(inside,) * 3,
            scratch_shapes=[
                pltpu.SMEM((4,), f32),
                pltpu.SMEM((4,), f32),
                pltpu.SMEM((4,), f32),
                pltpu.VMEM((6, 12, ROWS, 128), f32),
                pltpu.VMEM((10, ROWS, 128), f32),
                pltpu.VMEM((10, 8, 128), jnp.int32),
                pltpu.VMEM((3, 8, 8, 128), f32),
                pltpu.VMEM((2, 14, 8, 128), f32),
                pltpu.VMEM((2, 14, 8, 128), f32),
                pltpu.VMEM((3, 8, 128), f32),
                pltpu.VMEM((2, 2, 8, 128), f32),
                pltpu.VMEM((2, 2, 1, 8, 128), f32),
                pltpu.VMEM((2, 2, 2, 8, 128), f32),
                pltpu.VMEM((2, 2, 8, 128), f32),
                pltpu.VMEM((2, 2, 8, 128), f32),
                pltpu.VMEM((6, 6, 10, ROWS, 128), f32),
                pltpu.VMEM((3, 8, 8, 128), f32),
                pltpu.VMEM((sizes[2], 1, 128), f32),
                pltpu.VMEM((sizes[0] * sizes[1], 1, 128), f32),
                pltpu.SemaphoreType.DMA((4,)),
                pltpu.SemaphoreType.DMA((18,)),
                pltpu.SemaphoreType.DMA((22,)),
                pltpu.SemaphoreType.DMA((2,)),
                pltpu.SemaphoreType.REGULAR((2, 3)),
            ],
            compiler_params=pltpu.CompilerParams(
                collective_id=0, has_side_effects=True, vmem_limit_bytes=16 * 1024 * 1024
            ),
            name="line_search",
        )(*args)
        return pl.pallas_call(
            write_out,
            out_shape=outputs,
            in_specs=[inside] * 3,
            out_specs=(anywhere,) * 3,
            scratch_shapes=[pltpu.SemaphoreType.DMA((3,))],
            compiler_params=pltpu.CompilerParams(vmem_limit_bytes=4 * 1024 * 1024),
            name="write_out",
        )(*found)

    vector, scalar = P(None, "gx", "gy", "gz"), P("gx", "gy", "gz")
    return jax.shard_map(
        body,
        mesh=mesh,
        in_specs=(vector, vector, scalar, vector, scalar, P(), P(), P(), P()),
        out_specs=(P(), vector, vector),
        check_vma=False,
    )
```

```python
import functools

import jax
import jax.numpy as jnp
from jax import lax
from jax.experimental import pallas as pl
from jax.experimental.pallas import tpu as pltpu
from jax.sharding import PartitionSpec as P

MESH = pl.DeviceIdType.MESH
LENGTHS = (1.0, 0.5, 0.25, 0.125)
ROWS = 24
TOP = 8
TOGETHER = 6
ALONG = ((0, 3, 4), (3, 1, 5), (4, 5, 2))


def roll(values, shift, axis):
    return pltpu.roll(values, shift % values.shape[axis], axis)


def reach(size, far):
    return sorted((k for k in range(1, size) if min(k, size - k) <= far), key=lambda k: min(k, size - k))


def doubling(step, end):
    found = []
    while step < end:
        found.append(step)
        step *= 2
    return found


def take_rows(ref, start, row):
    return ref.reshape(ref.shape[0] * ROWS, 128)[pl.ds(start * ROWS + row, 8, stride=ROWS), :]


def put_rows(ref, start, row, value):
    ref.reshape(ref.shape[0] * ROWS, 128)[pl.ds(start * ROWS + row, 8, stride=ROWS), :] = value


def kernel(
    sizes,
    v_hbm, d_hbm, p_hbm, b_hbm, ph_hbm, fac_hbm, exp_hbm, yld_hbm, acc_ref,
    norms_ref, CV, CR,
    fac_ref, exp_ref, yld_ref, VP, PP, HP, BF, YS, YR, WS, ZR, XZ, YZ, ES, ER, SS, PR, RZ, RP,
    load_sem, send_sem, recv_sem, sum_sem, know_sem,
):
    n = dict(zip(("gx", "gy", "gz"), sizes))
    me = {a: lax.axis_index(a) for a in n}
    has = {}
    for a in n:
        has[a, 1] = me[a] < n[a] - 1
        has[a, -1] = me[a] > 0
    f32 = jnp.float32
    lane = lax.broadcasted_iota(jnp.int32, (8, 128), 1)
    sub = lax.broadcasted_iota(jnp.int32, (8, 128), 0)
    odd = (lane & 1) == 1
    first_lane, last_lane = lane == 0, lane == 127

    block = pl.ds(TOP, 8)
    loads = [
        pltpu.make_async_copy(v_hbm, VP.at[pl.ds(0, 3), pl.ds(2, 8), block], send_sem.at[0]),
        pltpu.make_async_copy(d_hbm, VP.at[pl.ds(3, 3), pl.ds(2, 8), block], send_sem.at[1]),
        pltpu.make_async_copy(p_hbm, PP.at[pl.ds(1, 8), block], send_sem.at[2]),
        pltpu.make_async_copy(ph_hbm, HP.at[pl.ds(1, 8)], send_sem.at[3]),
        pltpu.make_async_copy(b_hbm, BF, load_sem.at[0]),
        pltpu.make_async_copy(fac_hbm, fac_ref, load_sem.at[1]),
        pltpu.make_async_copy(exp_hbm, exp_ref, load_sem.at[2]),
        pltpu.make_async_copy(yld_hbm, yld_ref, load_sem.at[3]),
    ]
    for load in loads:
        load.start()

    zero = jnp.zeros((8, 128), f32)
    for c in range(6):
        for x in (0, 1, 10, 11):
            VP[c, x, block] = zero
    for x in (0, 9):
        PP[x, block] = zero
        HP[x] = jnp.zeros((8, 128), jnp.int32)
    for ref in (YR, ZR, XZ, YZ, ER):
        ref[...] = jnp.zeros(ref.shape, f32)

    groups = []

    def group(size):
        groups.append((len(groups), size, []))
        return groups[-1]

    def remote(src, dst, g, step):
        return pltpu.make_async_remote_copy(
            src_ref=src, dst_ref=dst, send_sem=send_sem.at[g], recv_sem=recv_sem.at[g],
            device_id={a: me[a] + s for a, s in step.items()}, device_id_type=MESH,
        )

    def message(into, step, pairs):
        send = functools.reduce(jnp.logical_and, [has[a, s] for a, s in step.items()])
        recv = functools.reduce(jnp.logical_and, [has[a, -s] for a, s in step.items()])
        into[2].append((send, recv, step, [remote(src, dst, into[0], step) for src, dst in pairs]))

    def start(into):
        for send, _, _, copies in into[2]:
            @pl.when(send)
            def _():
                for copy in copies:
                    copy.start()

    def wait_all(into, which):
        g, size, messages = into
        count = sum(m[which].astype(jnp.int32) for m in messages)
        for k in (1, 2, 4):
            if k <= len(messages):
                @pl.when(count == k)
                def _():
                    some = YS.at[0, pl.ds(0, k * size)]
                    whole = remote(some, some, g, messages[0][2])
                    if which:
                        whole.wait_recv()
                    else:
                        whole.wait_send()

    def arrived(into):
        wait_all(into, 1)

    def sent():
        for into in groups:
            wait_all(into, 0)

    both = (1, -1)
    hi = lambda s: (s + 1) // 2
    lo = lambda s: (1 - s) // 2
    x_near, x_far, y_near, y_far = (group(7) for _ in range(4))
    z_face, xz_edge, yz_edge, xy_edge = group(2), group(1), group(2), group(1)
    for s in both:
        near_from, near_to = (9, 1) if s == 1 else (2, 10)
        far_from, far_to = (8, 0) if s == 1 else (3, 11)
        p_from, p_to = (8, 0) if s == 1 else (1, 9)
        message(x_near, {"gx": s}, [
            (VP.at[:, near_from, block], VP.at[:, near_to, block]),
            (PP.at[p_from, block], PP.at[p_to, block]),
        ])
        message(x_far, {"gx": s}, [
            (VP.at[:, far_from, block], VP.at[:, far_to, block]),
            (HP.at[p_from], HP.at[p_to]),
        ])
        message(y_near, {"gy": s}, [(YS.at[hi(s), pl.ds(0, 7)], YR.at[lo(s), pl.ds(0, 7)])])
        message(y_far, {"gy": s}, [(YS.at[hi(s), pl.ds(7, 7)], YR.at[lo(s), pl.ds(7, 7)])])
        message(z_face, {"gz": s}, [(WS.at[pl.ds(0, 2)], ZR.at[lo(s)])])
        for t in both:
            message(xz_edge, {"gx": s, "gz": t}, [(WS.at[pl.ds(1, 1)], XZ.at[lo(s), lo(t)])])
            message(yz_edge, {"gy": s, "gz": t}, [(WS.at[pl.ds(1, 2)], YZ.at[lo(s), lo(t)])])
            message(xy_edge, {"gx": s, "gy": t}, [(ES.at[hi(s), hi(t)], ER.at[lo(s), lo(t)])])

    barrier = pltpu.get_barrier_semaphore()

    greeted = {"gz": reach(n["gz"], 2), "gy": reach(n["gy"], 2)}

    def signal(sem, a, k):
        pl.semaphore_signal(sem, inc=1, device_id={a: lax.rem(me[a] + k, n[a])}, device_id_type=MESH)

    def signal_x(sem, step):
        for s in (step, -step):
            there = jnp.logical_and(me["gx"] + s >= 0, me["gx"] + s < n["gx"])

            @pl.when(there)
            def _():
                pl.semaphore_signal(sem, inc=1, device_id={"gx": me["gx"] + s}, device_id_type=MESH)

    def count_x(step):
        return (me["gx"] + step < n["gx"]).astype(jnp.int32) + (me["gx"] - step >= 0).astype(jnp.int32)

    for a, b in (("gx", "gy"), ("gx", "gz"), ("gy", "gz")):
        for s in both:
            for t in both:
                @pl.when(jnp.logical_and(has[a, s], has[b, t]))
                def _():
                    pl.semaphore_signal(
                        barrier, inc=1, device_id={a: me[a] + s, b: me[b] + t}, device_id_type=MESH
                    )
    for a in greeted:
        for k in greeted[a]:
            signal(barrier, a, k)
    signal_x(barrier, 1)
    sides = {a: has[a, 1].astype(jnp.int32) + has[a, -1].astype(jnp.int32) for a in n}
    edges = sides["gx"] * sides["gy"] + sides["gx"] * sides["gz"] + sides["gy"] * sides["gz"]

    z_rounds = doubling(2, n["gz"] // 2)
    x_rounds = doubling(1, n["gx"])

    def tell_z(r):
        if r < len(z_rounds):
            for k in (z_rounds[r], n["gz"] - z_rounds[r]):
                signal(know_sem.at[0, r], "gz", k)

    def told_z(r):
        if r < len(z_rounds):
            pl.semaphore_wait(know_sem.at[0, r], 2)

    def tell_x(r):
        if r < len(x_rounds):
            signal_x(know_sem.at[1, r], x_rounds[r])

    def told_x(r):
        if r < len(x_rounds):
            pl.semaphore_wait(know_sem.at[1, r], count_x(x_rounds[r]))

    for load in loads[:4]:
        load.wait()

    def y_layer(c, y):
        return take_rows(VP.at[c], 2, TOP + y)

    for side, near, far in ((0, 0, 1), (1, 7, 6)):
        for c in range(6):
            YS[side, c] = y_layer(c, near)
            YS[side, 8 + c] = y_layer(c, far)
        YS[side, 6] = take_rows(PP, 1, TOP + near)
        YS[side, 7] = HP[pl.ds(1, 8), near, :].astype(f32)
        for s, xp in ((0, 2), (1, 9)):
            for c in range(6):
                ES[s, side, pl.ds(c, 1)] = VP[c, xp, pl.ds(TOP + near, 1)]

    pair = lane >> 1
    outer = jnp.where(odd, (lane + 1) >> 1, (lane >> 1) - 1) & 63
    near_z, far_z = zero, zero
    for c in range(8):
        one, two = zero, zero
        for x in range(8):
            if c < 6:
                plane = VP[c, x + 2, block]
            elif c == 6:
                plane = PP[x + 1, block]
            else:
                plane = HP[x + 1].astype(f32)
            k = 8 * c + x
            turned = roll(plane, 2 * k + 1, 1)
            one = jnp.where(pair == k, turned, one)
            if c < 6:
                two = jnp.where(outer == k, turned, two)
        near_z = jnp.where((lane >> 4) == c, one, near_z)
        if c < 6:
            far_z = jnp.where((outer >> 3) == c, two, far_z)
    WS[0] = far_z
    WS[1] = near_z
    near_zy = zero
    for side in range(2):
        for c in range(6):
            k = 8 * side + c
            near_zy = jnp.where(pair == k, roll(YS[side, c], 2 * k + 1, 1), near_zy)
    WS[2] = near_zy

    pl.semaphore_wait(barrier, sum(len(ks) for ks in greeted.values()) + sides["gx"] + edges)
    for into in (z_face, xz_edge, yz_edge, xy_edge, x_near, y_near, x_far, y_far):
        start(into)
    tell_z(0)
    tell_x(0)

    for load in loads[5:]:
        load.wait()
    picked = acc_ref[0]
    length = jnp.where(
        picked == 0, f32(1.0), jnp.where(picked == 1, f32(0.5), jnp.where(picked == 2, f32(0.25), f32(0.125)))
    )
    for c in range(3):
        for x in range(8):
            CV[c, x] = VP[c, x + 2, block] + length * VP[3 + c, x + 2, block]

    full = lambda s: jnp.full((8, 128), s, f32)
    table = []
    for k in range(4):
        exponent = full(exp_ref[k])
        table.append((full(fac_ref[k]), (1.0 - exponent) / (2.0 * exponent), full(0.5 * yld_ref[k])))

    def params(ids):
        out = table[3]
        for k in (2, 1, 0):
            hit = ids == k
            out = tuple(jnp.where(hit, mine, other) for mine, other in zip(table[k], out))
        return out

    for x in range(8):
        for i, value in enumerate(params(HP[x + 1])):
            PR[i, x] = value

    def tensor(g):
        return (
            g[0][0], g[1][1], g[2][2],
            0.5 * (g[0][1] + g[1][0]), 0.5 * (g[0][2] + g[2][0]), 0.5 * (g[1][2] + g[2][1]),
        )

    def dot(a, b):
        return (a[0] * b[0] + a[1] * b[1] + a[2] * b[2]) + 2.0 * (a[3] * b[3] + a[4] * b[4] + a[5] * b[5])

    def flow(second, factor, power, half_yield):
        inverse = lax.rsqrt(second)
        creep = factor * jnp.exp(power * jnp.log(second))
        plastic = half_yield * inverse
        total = creep + plastic
        return inverse, creep, plastic, total, creep * plastic / total

    def stresses(g, material, wanted, mask=None):
        factor, power, half_yield = material
        base, change = tensor(g[:3]), tensor(g[3:])
        inverse, creep, plastic, total, harmonic = flow(0.125 * dot(base, base) + 0.01, factor, power, half_yield)
        viscosity = 0.5 * harmonic + 0.025
        slope = harmonic * (inverse * inverse) * (plastic * power - 0.5 * creep) / total
        along = slope * (0.125 * dot(base, change))
        if mask is not None:
            viscosity, along = viscosity * mask, along * mask
        fields = [
            {c: viscosity * base[c] for c in wanted},
            {c: viscosity * change[c] + along * base[c] for c in wanted},
        ]
        for a in LENGTHS:
            trial = tuple(e + f if a == 1.0 else e + a * f for e, f in zip(base, change))
            viscosity = 0.5 * flow(0.125 * dot(trial, trial) + 0.01, factor, power, half_yield)[4] + 0.025
            if mask is not None:
                viscosity = viscosity * mask
            fields.append({c: viscosity * trial[c] for c in wanted})
        return fields

    def across_z(plane, ends):
        return jnp.where(last_lane, ends, roll(plane, -1, 1)) - jnp.where(first_lane, ends, roll(plane, 1, 1))

    def ends_of(packed, k):
        return pltpu.roll(packed, 127 - 2 * k, 1)

    def joined(below, above):
        return jnp.where(odd, roll(below, 1, 1), roll(above, -1, 1))

    def flag(a, s):
        return has[a, s].astype(f32)

    def plane_differences(xp, packed, x):
        g = []
        for c in range(6):
            centre = VP[c, xp, block]
            g.append((
                VP[c, xp + 1, block] - VP[c, xp - 1, block],
                VP[c, xp, pl.ds(TOP + 1, 8)] - VP[c, xp, pl.ds(TOP - 1, 8)],
                across_z(centre, ends_of(packed, 8 * c + x)),
            ))
        return g

    every = tuple(range(6))

    def store_plane(xs, fields):
        for f, field in enumerate(fields):
            for c, value in field.items():
                SS[f, c, xs, block] = value

    told_z(0)
    tell_z(1)
    told_x(0)
    tell_x(1)
    arrived(z_face)
    arrived(y_near)
    near_halo = joined(ZR[0, 1], ZR[1, 1])
    far_halo = jnp.where(odd, roll(ZR[0, 0], 2, 1), roll(ZR[1, 0], -2, 1))
    for side, row in ((0, TOP - 1), (1, TOP + 8)):
        for c in range(6):
            put_rows(VP.at[c], 2, row, YR[side, c])
        put_rows(PP, 1, row, YR[side, 6])

    def own_plane(x):
        material = tuple(PR[i, x] for i in range(3))
        store_plane(x + 1, stresses(plane_differences(x + 2, near_halo, x), material, every))

    def some_planes(i, carry):
        for k in range(TOGETHER):
            own_plane(1 + TOGETHER * i + k)
        return carry

    lax.fori_loop(0, 6 // TOGETHER, some_planes, 0)

    arrived(x_near)
    own_plane(0)
    own_plane(7)
    arrived(xz_edge)
    arrived(yz_edge)
    x_ends = [joined(XZ[side, 0, 0], XZ[side, 1, 0]) for side in range(2)]
    inner = WS[1]
    y_ends = [joined(YZ[side, 0, 0], YZ[side, 1, 0]) for side in range(2)]
    column = pair & 7
    out_z = jnp.where(odd, inner - far_halo, far_halo - inner)
    out_y = roll(jnp.where(sub == 0, y_ends[1], near_halo), -1, 0) - roll(
        jnp.where(sub == 7, y_ends[0], near_halo), 1, 0
    )
    out_x = jnp.where(column == 7, roll(x_ends[1], 14, 1), roll(near_halo, -2, 1)) - jnp.where(
        column == 0, roll(x_ends[0], -14, 1), roll(near_halo, 2, 1)
    )
    g = [tuple(roll(o, -16 * c, 1) if c else o for o in (out_x, out_y, out_z)) for c in range(6)]
    mask = jnp.where(odd, flag("gz", -1), flag("gz", 1))
    z_fields = stresses(g, params(roll(near_halo, -112, 1)), ALONG[2], mask)

    arrived(xy_edge)
    arrived(y_far)
    for side in range(2):
        packed = joined(YZ[side, 0, 1], YZ[side, 1, 1])
        g = []
        for c in range(6):
            centre = YR[side, c]
            above = jnp.where(sub == 7, ER[1, side, pl.ds(c, 1)], roll(centre, -1, 0))
            below = jnp.where(sub == 0, ER[0, side, pl.ds(c, 1)], roll(centre, 1, 0))
            outward = YS[side, c] - YR[side, 8 + c]
            g.append((
                above - below,
                outward if side == 0 else -outward,
                across_z(centre, ends_of(packed, 8 * (1 - side) + c)),
            ))
        fields = stresses(g, params(YR[side, 7]), ALONG[1], flag("gy", 2 * side - 1))
        row = TOP - 1 if side == 0 else TOP + 8
        for f, field in enumerate(fields):
            for c, value in field.items():
                put_rows(SS.at[f, c], 1, row, value)

    for s, xp in ((0, 1), (1, 10)):
        for t, row in ((0, TOP - 1), (1, TOP + 8)):
            for c in range(6):
                VP[c, xp, pl.ds(row, 1)] = ER[s, t, pl.ds(c, 1)]
    arrived(x_far)
    for side, xp, x in ((0, 1, 7), (1, 10, 0)):
        g = plane_differences(xp, x_ends[side], x)
        store_plane(xp - 1, stresses(g, params(HP[xp - 1]), ALONG[0], flag("gx", 2 * side - 1)))

    for r in range(1, len(z_rounds)):
        told_z(r)
        tell_z(r + 1)
    told_x(1)
    tell_x(2)

    loads[4].wait()
    sums = [zero] * 8
    for x in range(8):
        xs = x + 1
        p_plane = PP[xs, block]
        slope = (
            PP[xs + 1, block] - PP[xs - 1, block],
            PP[xs, pl.ds(TOP + 1, 8)] - PP[xs, pl.ds(TOP - 1, 8)],
            across_z(p_plane, ends_of(near_halo, 48 + x)),
        )
        for i in range(3):
            loading = BF[i, x] - 0.5 * slope[i]
            cx, cy, cz = ALONG[0][i], ALONG[1][i], ALONG[2][i]
            out = []
            for f in range(6):
                change = SS[f, cx, xs + 1, block] - SS[f, cx, xs - 1, block]
                change = change + (SS[f, cy, xs, pl.ds(TOP + 1, 8)] - SS[f, cy, xs, pl.ds(TOP - 1, 8)])
                change = change + across_z(SS[f, cz, xs, block], ends_of(z_fields[f][cz], x))
                out.append(change if f == 1 else change + loading)
            chosen = out[5]
            for k in (2, 1, 0):
                chosen = jnp.where(picked == k, out[2 + k], chosen)
            CR[i, x] = chosen
            for k, a in enumerate(LENGTHS):
                sums[k] = sums[k] + out[2 + k] * out[2 + k]
                linear = out[0] + a * out[1]
                sums[4 + k] = sums[4 + k] + linear * linear

    stacked = zero
    for k in range(8):
        stacked = jnp.where(sub == k, jnp.sum(sums[k], axis=0, keepdims=True), stacked)
    totals = jnp.sum(stacked, axis=1, keepdims=True)
    row = jnp.sum(jnp.where(lane == sub, totals, 0.0), axis=0, keepdims=True)
    for stage, (axes, ref) in enumerate(((("gz",), RZ), (("gx", "gy"), RP))):
        offsets = [()]
        for a in axes:
            offsets = [o + (k,) for o in offsets for k in range(n[a])]
        hops = lambda o: sum(min(k, n[a] - k) for k, a in zip(o, axes))
        mine = 0
        for a in axes:
            mine = mine * n[a] + me[a]
        if len(axes) == 2:
            for r in range(2, len(x_rounds)):
                told_x(r)
                tell_x(r + 1)
        ref[mine] = row

        def share(rows, target):
            return pltpu.make_async_remote_copy(
                src_ref=rows, dst_ref=rows, send_sem=load_sem.at[stage], recv_sem=sum_sem.at[stage],
                device_id=target, device_id_type=MESH,
            )

        others = sorted((o for o in offsets if any(o)), key=lambda o: -hops(o))
        targets = [{a: lax.rem(me[a] + k, n[a]) for k, a in zip(o, axes)} for o in others]
        for target in targets:
            share(ref.at[mine], target).start()
        if stage == 0:
            sent()
        whole = share(ref.at[pl.ds(0, len(others))], targets[0])
        whole.wait_send()
        whole.wait_recv()
        rows = [ref[k] for k in range(len(offsets))]
        while len(rows) > 1:
            rows = [sum(rows[k:k + 2]) for k in range(0, len(rows), 2)]
        row = rows[0]
    cells = 3.0 * (8 * n["gx"]) * (8 * n["gy"]) * (128 * n["gz"])
    norms = jnp.sqrt(row / cells + 1e-6)
    norms_ref[pl.ds(0, 1)] = norms[:, 0:4]
    norms_ref[pl.ds(1, 1)] = roll(jnp.broadcast_to(norms, (8, 128)), -4, 1)[0:1, 0:4]


def write_out(*refs):
    copies = [pltpu.make_async_copy(refs[i], refs[3 + i], refs[6].at[i]) for i in range(3)]
    for copy in copies:
        copy.start()
    for copy in copies:
        copy.wait()


def solution(mesh):
    sizes = tuple(mesh.shape[a] for a in ("gx", "gy", "gz"))
    f32 = jnp.float32

    def body(*args):
        vector = jax.ShapeDtypeStruct((3, 8, 8, 128), f32)
        anywhere = pl.BlockSpec(memory_space=pl.ANY)
        inside = pl.BlockSpec(memory_space=pltpu.VMEM)
        args = [pltpu.with_memory_space_constraint(a, pltpu.HBM) for a in args[:8]] + [args[8]]
        outputs = (jax.ShapeDtypeStruct((2, 4), f32), vector, vector)
        found = pl.pallas_call(
            functools.partial(kernel, sizes),
            out_shape=outputs,
            in_specs=[pl.BlockSpec(memory_space=pltpu.HBM)] * 8 + [pl.BlockSpec(memory_space=pltpu.SMEM)],
            out_specs=(inside,) * 3,
            scratch_shapes=[
                pltpu.SMEM((4,), f32),
                pltpu.SMEM((4,), f32),
                pltpu.SMEM((4,), f32),
                pltpu.VMEM((6, 12, ROWS, 128), f32),
                pltpu.VMEM((10, ROWS, 128), f32),
                pltpu.VMEM((10, 8, 128), jnp.int32),
                pltpu.VMEM((3, 8, 8, 128), f32),
                pltpu.VMEM((2, 14, 8, 128), f32),
                pltpu.VMEM((2, 14, 8, 128), f32),
                pltpu.VMEM((3, 8, 128), f32),
                pltpu.VMEM((2, 2, 8, 128), f32),
                pltpu.VMEM((2, 2, 1, 8, 128), f32),
                pltpu.VMEM((2, 2, 2, 8, 128), f32),
                pltpu.VMEM((2, 2, 8, 128), f32),
                pltpu.VMEM((2, 2, 8, 128), f32),
                pltpu.VMEM((6, 6, 10, ROWS, 128), f32),
                pltpu.VMEM((3, 8, 8, 128), f32),
                pltpu.VMEM((sizes[2], 1, 128), f32),
                pltpu.VMEM((sizes[0] * sizes[1], 1, 128), f32),
                pltpu.SemaphoreType.DMA((4,)),
                pltpu.SemaphoreType.DMA((8,)),
                pltpu.SemaphoreType.DMA((8,)),
                pltpu.SemaphoreType.DMA((2,)),
                pltpu.SemaphoreType.REGULAR((2, 3)),
            ],
            compiler_params=pltpu.CompilerParams(
                collective_id=0, has_side_effects=True, vmem_limit_bytes=16 * 1024 * 1024
            ),
            name="line_search",
        )(*args)
        return pl.pallas_call(
            write_out,
            out_shape=outputs,
            in_specs=[inside] * 3,
            out_specs=(anywhere,) * 3,
            scratch_shapes=[pltpu.SemaphoreType.DMA((3,))],
            compiler_params=pltpu.CompilerParams(vmem_limit_bytes=4 * 1024 * 1024),
            name="write_out",
        )(*found)

    vector, scalar = P(None, "gx", "gy", "gz"), P("gx", "gy", "gz")
    return jax.shard_map(
        body,
        mesh=mesh,
        in_specs=(vector, vector, scalar, vector, scalar, P(), P(), P(), P()),
        out_specs=(P(), vector, vector),
        check_vma=False,
    )
```

```python
import functools

import jax
import jax.numpy as jnp
from jax import lax
from jax.experimental import pallas as pl
from jax.experimental.pallas import tpu as pltpu
from jax.sharding import PartitionSpec as P

MESH = pl.DeviceIdType.MESH
LENGTHS = (1.0, 0.5, 0.25, 0.125)
ROWS = 24
TOP = 8
TOGETHER = 6
ALONG = ((0, 3, 4), (3, 1, 5), (4, 5, 2))


def roll(values, shift, axis):
    return pltpu.roll(values, shift % values.shape[axis], axis)


def reach(size, far):
    return sorted((k for k in range(1, size) if min(k, size - k) <= far), key=lambda k: min(k, size - k))


def doubling(step, end):
    found = []
    while step < end:
        found.append(step)
        step *= 2
    return found


def take_rows(ref, start, row):
    return ref.reshape(ref.shape[0] * ROWS, 128)[pl.ds(start * ROWS + row, 8, stride=ROWS), :]


def put_rows(ref, start, row, value):
    ref.reshape(ref.shape[0] * ROWS, 128)[pl.ds(start * ROWS + row, 8, stride=ROWS), :] = value


def kernel(
    sizes,
    v_hbm, d_hbm, p_hbm, b_hbm, ph_hbm, fac_hbm, exp_hbm, yld_hbm, acc_ref,
    norms_ref, CV, CR,
    fac_ref, exp_ref, yld_ref, VP, PP, HP, BF, YS, YR, WS, ZR, XZ, YZ, ES, ER, SS, PR, RZ, RP,
    load_sem, send_sem, recv_sem, sum_sem, know_sem,
):
    n = dict(zip(("gx", "gy", "gz"), sizes))
    me = {a: lax.axis_index(a) for a in n}
    has = {}
    for a in n:
        has[a, 1] = me[a] < n[a] - 1
        has[a, -1] = me[a] > 0
    f32 = jnp.float32
    lane = lax.broadcasted_iota(jnp.int32, (8, 128), 1)
    sub = lax.broadcasted_iota(jnp.int32, (8, 128), 0)
    odd = (lane & 1) == 1
    first_lane, last_lane = lane == 0, lane == 127

    block = pl.ds(TOP, 8)
    loads = [
        pltpu.make_async_copy(v_hbm, VP.at[pl.ds(0, 3), pl.ds(2, 8), block], send_sem.at[0]),
        pltpu.make_async_copy(d_hbm, VP.at[pl.ds(3, 3), pl.ds(2, 8), block], send_sem.at[1]),
        pltpu.make_async_copy(p_hbm, PP.at[pl.ds(1, 8), block], send_sem.at[2]),
        pltpu.make_async_copy(ph_hbm, HP.at[pl.ds(1, 8)], send_sem.at[3]),
        pltpu.make_async_copy(b_hbm, BF, load_sem.at[0]),
        pltpu.make_async_copy(fac_hbm, fac_ref, load_sem.at[1]),
        pltpu.make_async_copy(exp_hbm, exp_ref, load_sem.at[2]),
        pltpu.make_async_copy(yld_hbm, yld_ref, load_sem.at[3]),
    ]
    for load in loads:
        load.start()

    zero = jnp.zeros((8, 128), f32)
    for c in range(6):
        for x in (0, 1, 10, 11):
            VP[c, x, block] = zero
    for x in (0, 9):
        PP[x, block] = zero
        HP[x] = jnp.zeros((8, 128), jnp.int32)
    for ref in (YR, ZR, XZ, YZ, ER):
        ref[...] = jnp.zeros(ref.shape, f32)

    groups = []

    def group(size):
        groups.append((len(groups), size, []))
        return groups[-1]

    def remote(src, dst, g, step):
        return pltpu.make_async_remote_copy(
            src_ref=src, dst_ref=dst, send_sem=send_sem.at[g], recv_sem=recv_sem.at[g],
            device_id={a: me[a] + s for a, s in step.items()}, device_id_type=MESH,
        )

    def message(into, step, pairs):
        send = functools.reduce(jnp.logical_and, [has[a, s] for a, s in step.items()])
        recv = functools.reduce(jnp.logical_and, [has[a, -s] for a, s in step.items()])
        into[2].append((send, recv, step, [remote(src, dst, into[0], step) for src, dst in pairs]))

    def start(into):
        for send, _, _, copies in into[2]:
            @pl.when(send)
            def _():
                for copy in copies:
                    copy.start()

    def wait_all(into, which):
        g, size, messages = into
        count = sum(m[which].astype(jnp.int32) for m in messages)
        for k in (1, 2, 4):
            if k <= len(messages):
                @pl.when(count == k)
                def _():
                    some = YS.at[0, pl.ds(0, k * size)]
                    whole = remote(some, some, g, messages[0][2])
                    if which:
                        whole.wait_recv()
                    else:
                        whole.wait_send()

    def arrived(into):
        wait_all(into, 1)

    def sent():
        for into in groups:
            wait_all(into, 0)

    both = (1, -1)
    hi = lambda s: (s + 1) // 2
    lo = lambda s: (1 - s) // 2
    x_near, x_far, y_near, y_far = (group(7) for _ in range(4))
    z_face, xz_edge, yz_edge, xy_edge = group(2), group(1), group(2), group(1)
    for s in both:
        near_from, near_to = (9, 1) if s == 1 else (2, 10)
        far_from, far_to = (8, 0) if s == 1 else (3, 11)
        p_from, p_to = (8, 0) if s == 1 else (1, 9)
        message(x_near, {"gx": s}, [
            (VP.at[:, near_from, block], VP.at[:, near_to, block]),
            (PP.at[p_from, block], PP.at[p_to, block]),
        ])
        message(x_far, {"gx": s}, [
            (VP.at[:, far_from, block], VP.at[:, far_to, block]),
            (HP.at[p_from], HP.at[p_to]),
        ])
        message(y_near, {"gy": s}, [(YS.at[hi(s), pl.ds(0, 7)], YR.at[lo(s), pl.ds(0, 7)])])
        message(y_far, {"gy": s}, [(YS.at[hi(s), pl.ds(7, 7)], YR.at[lo(s), pl.ds(7, 7)])])
        message(z_face, {"gz": s}, [(WS.at[pl.ds(0, 2)], ZR.at[lo(s)])])
        for t in both:
            message(xz_edge, {"gx": s, "gz": t}, [(WS.at[pl.ds(1, 1)], XZ.at[lo(s), lo(t)])])
            message(yz_edge, {"gy": s, "gz": t}, [(WS.at[pl.ds(1, 2)], YZ.at[lo(s), lo(t)])])
            message(xy_edge, {"gx": s, "gy": t}, [(ES.at[hi(s), hi(t)], ER.at[lo(s), lo(t)])])

    barrier = pltpu.get_barrier_semaphore()

    greeted = {"gz": reach(n["gz"], 2), "gy": reach(n["gy"], 2)}

    def signal(sem, a, k):
        pl.semaphore_signal(sem, inc=1, device_id={a: lax.rem(me[a] + k, n[a])}, device_id_type=MESH)

    def signal_x(sem, step):
        for s in (step, -step):
            there = jnp.logical_and(me["gx"] + s >= 0, me["gx"] + s < n["gx"])

            @pl.when(there)
            def _():
                pl.semaphore_signal(sem, inc=1, device_id={"gx": me["gx"] + s}, device_id_type=MESH)

    def count_x(step):
        return (me["gx"] + step < n["gx"]).astype(jnp.int32) + (me["gx"] - step >= 0).astype(jnp.int32)

    for a, b in (("gx", "gy"), ("gx", "gz"), ("gy", "gz")):
        for s in both:
            for t in both:
                @pl.when(jnp.logical_and(has[a, s], has[b, t]))
                def _():
                    pl.semaphore_signal(
                        barrier, inc=1, device_id={a: me[a] + s, b: me[b] + t}, device_id_type=MESH
                    )
    for a in greeted:
        for k in greeted[a]:
            signal(barrier, a, k)
    signal_x(barrier, 1)
    sides = {a: has[a, 1].astype(jnp.int32) + has[a, -1].astype(jnp.int32) for a in n}
    edges = sides["gx"] * sides["gy"] + sides["gx"] * sides["gz"] + sides["gy"] * sides["gz"]

    z_rounds = doubling(2, n["gz"] // 2)
    x_rounds = doubling(1, n["gx"])

    def tell_z(r):
        if r < len(z_rounds):
            for k in (z_rounds[r], n["gz"] - z_rounds[r]):
                signal(know_sem.at[0, r], "gz", k)

    def told_z(r):
        if r < len(z_rounds):
            pl.semaphore_wait(know_sem.at[0, r], 2)

    def tell_x(r):
        if r < len(x_rounds):
            signal_x(know_sem.at[1, r], x_rounds[r])

    def told_x(r):
        if r < len(x_rounds):
            pl.semaphore_wait(know_sem.at[1, r], count_x(x_rounds[r]))

    for load in loads[:4]:
        load.wait()

    def y_layer(c, y):
        return take_rows(VP.at[c], 2, TOP + y)

    for side, near, far in ((0, 0, 1), (1, 7, 6)):
        for c in range(6):
            YS[side, c] = y_layer(c, near)
            YS[side, 8 + c] = y_layer(c, far)
        YS[side, 6] = take_rows(PP, 1, TOP + near)
        YS[side, 7] = HP[pl.ds(1, 8), near, :].astype(f32)
        for s, xp in ((0, 2), (1, 9)):
            for c in range(6):
                ES[s, side, pl.ds(c, 1)] = VP[c, xp, pl.ds(TOP + near, 1)]

    pair = lane >> 1
    outer = jnp.where(odd, (lane + 1) >> 1, (lane >> 1) - 1) & 63
    near_z, far_z = zero, zero
    for c in range(8):
        one, two = zero, zero
        for x in range(8):
            if c < 6:
                plane = VP[c, x + 2, block]
            elif c == 6:
                plane = PP[x + 1, block]
            else:
                plane = HP[x + 1].astype(f32)
            k = 8 * c + x
            turned = roll(plane, 2 * k + 1, 1)
            one = jnp.where(pair == k, turned, one)
            if c < 6:
                two = jnp.where(outer == k, turned, two)
        near_z = jnp.where((lane >> 4) == c, one, near_z)
        if c < 6:
            far_z = jnp.where((outer >> 3) == c, two, far_z)
    WS[0] = far_z
    WS[1] = near_z
    near_zy = zero
    for side in range(2):
        for c in range(6):
            k = 8 * side + c
            near_zy = jnp.where(pair == k, roll(YS[side, c], 2 * k + 1, 1), near_zy)
    WS[2] = near_zy

    pl.semaphore_wait(barrier, sum(len(ks) for ks in greeted.values()) + sides["gx"] + edges)
    for into in (z_face, xz_edge, yz_edge, xy_edge, x_near, y_near, x_far, y_far):
        start(into)
    tell_z(0)
    tell_x(0)

    for load in loads[5:]:
        load.wait()
    picked = acc_ref[0]
    length = jnp.where(
        picked == 0, f32(1.0), jnp.where(picked == 1, f32(0.5), jnp.where(picked == 2, f32(0.25), f32(0.125)))
    )
    for c in range(3):
        for x in range(8):
            CV[c, x] = VP[c, x + 2, block] + length * VP[3 + c, x + 2, block]

    full = lambda s: jnp.full((8, 128), s, f32)
    table = []
    for k in range(4):
        exponent = full(exp_ref[k])
        table.append((full(fac_ref[k]), (1.0 - exponent) / (2.0 * exponent), full(0.5 * yld_ref[k])))

    def params(ids):
        out = table[3]
        for k in (2, 1, 0):
            hit = ids == k
            out = tuple(jnp.where(hit, mine, other) for mine, other in zip(table[k], out))
        return out

    for x in range(8):
        for i, value in enumerate(params(HP[x + 1])):
            PR[i, x] = value

    def tensor(g):
        return (
            g[0][0], g[1][1], g[2][2],
            0.5 * (g[0][1] + g[1][0]), 0.5 * (g[0][2] + g[2][0]), 0.5 * (g[1][2] + g[2][1]),
        )

    def dot(a, b):
        return (a[0] * b[0] + a[1] * b[1] + a[2] * b[2]) + 2.0 * (a[3] * b[3] + a[4] * b[4] + a[5] * b[5])

    def flow(second, factor, power, half_yield):
        inverse = lax.rsqrt(second)
        creep = factor * jnp.exp(power * jnp.log(second))
        plastic = half_yield * inverse
        total = creep + plastic
        return inverse, creep, plastic, total, creep * plastic / total

    def stresses(g, material, wanted, mask=None):
        factor, power, half_yield = material
        base, change = tensor(g[:3]), tensor(g[3:])
        inverse, creep, plastic, total, harmonic = flow(0.125 * dot(base, base) + 0.01, factor, power, half_yield)
        viscosity = 0.5 * harmonic + 0.025
        slope = harmonic * (inverse * inverse) * (plastic * power - 0.5 * creep) / total
        along = slope * (0.125 * dot(base, change))
        if mask is not None:
            viscosity, along = viscosity * mask, along * mask
        fields = [
            {c: viscosity * base[c] for c in wanted},
            {c: viscosity * change[c] + along * base[c] for c in wanted},
        ]
        for a in LENGTHS:
            trial = tuple(e + f if a == 1.0 else e + a * f for e, f in zip(base, change))
            viscosity = 0.5 * flow(0.125 * dot(trial, trial) + 0.01, factor, power, half_yield)[4] + 0.025
            if mask is not None:
                viscosity = viscosity * mask
            fields.append({c: viscosity * trial[c] for c in wanted})
        return fields

    def across_z(plane, ends):
        return jnp.where(last_lane, ends, roll(plane, -1, 1)) - jnp.where(first_lane, ends, roll(plane, 1, 1))

    def ends_of(packed, k):
        return pltpu.roll(packed, 127 - 2 * k, 1)

    def joined(below, above):
        return jnp.where(odd, roll(below, 1, 1), roll(above, -1, 1))

    def flag(a, s):
        return has[a, s].astype(f32)

    def plane_differences(xp, packed, x):
        g = []
        for c in range(6):
            centre = VP[c, xp, block]
            g.append((
                VP[c, xp + 1, block] - VP[c, xp - 1, block],
                VP[c, xp, pl.ds(TOP + 1, 8)] - VP[c, xp, pl.ds(TOP - 1, 8)],
                across_z(centre, ends_of(packed, 8 * c + x)),
            ))
        return g

    every = tuple(range(6))

    def store_plane(xs, fields):
        for f, field in enumerate(fields):
            for c, value in field.items():
                SS[f, c, xs, block] = value

    arrived(z_face)
    arrived(y_near)
    near_halo = joined(ZR[0, 1], ZR[1, 1])
    far_halo = jnp.where(odd, roll(ZR[0, 0], 2, 1), roll(ZR[1, 0], -2, 1))
    for side, row in ((0, TOP - 1), (1, TOP + 8)):
        for c in range(6):
            put_rows(VP.at[c], 2, row, YR[side, c])
        put_rows(PP, 1, row, YR[side, 6])

    def own_plane(x):
        material = tuple(PR[i, x] for i in range(3))
        store_plane(x + 1, stresses(plane_differences(x + 2, near_halo, x), material, every))

    def some_planes(i, carry):
        for k in range(TOGETHER):
            own_plane(1 + TOGETHER * i + k)
        return carry

    lax.fori_loop(0, 6 // TOGETHER, some_planes, 0)
    told_z(0)
    tell_z(1)
    told_x(0)
    tell_x(1)

    arrived(x_near)
    own_plane(0)
    own_plane(7)
    arrived(xz_edge)
    arrived(yz_edge)
    x_ends = [joined(XZ[side, 0, 0], XZ[side, 1, 0]) for side in range(2)]
    inner = WS[1]
    y_ends = [joined(YZ[side, 0, 0], YZ[side, 1, 0]) for side in range(2)]
    column = pair & 7
    out_z = jnp.where(odd, inner - far_halo, far_halo - inner)
    out_y = roll(jnp.where(sub == 0, y_ends[1], near_halo), -1, 0) - roll(
        jnp.where(sub == 7, y_ends[0], near_halo), 1, 0
    )
    out_x = jnp.where(column == 7, roll(x_ends[1], 14, 1), roll(near_halo, -2, 1)) - jnp.where(
        column == 0, roll(x_ends[0], -14, 1), roll(near_halo, 2, 1)
    )
    g = [tuple(roll(o, -16 * c, 1) if c else o for o in (out_x, out_y, out_z)) for c in range(6)]
    mask = jnp.where(odd, flag("gz", -1), flag("gz", 1))
    z_fields = stresses(g, params(roll(near_halo, -112, 1)), ALONG[2], mask)

    arrived(xy_edge)
    arrived(y_far)
    for side in range(2):
        packed = joined(YZ[side, 0, 1], YZ[side, 1, 1])
        g = []
        for c in range(6):
            centre = YR[side, c]
            above = jnp.where(sub == 7, ER[1, side, pl.ds(c, 1)], roll(centre, -1, 0))
            below = jnp.where(sub == 0, ER[0, side, pl.ds(c, 1)], roll(centre, 1, 0))
            outward = YS[side, c] - YR[side, 8 + c]
            g.append((
                above - below,
                outward if side == 0 else -outward,
                across_z(centre, ends_of(packed, 8 * (1 - side) + c)),
            ))
        fields = stresses(g, params(YR[side, 7]), ALONG[1], flag("gy", 2 * side - 1))
        row = TOP - 1 if side == 0 else TOP + 8
        for f, field in enumerate(fields):
            for c, value in field.items():
                put_rows(SS.at[f, c], 1, row, value)

    for s, xp in ((0, 1), (1, 10)):
        for t, row in ((0, TOP - 1), (1, TOP + 8)):
            for c in range(6):
                VP[c, xp, pl.ds(row, 1)] = ER[s, t, pl.ds(c, 1)]
    arrived(x_far)
    for side, xp, x in ((0, 1, 7), (1, 10, 0)):
        g = plane_differences(xp, x_ends[side], x)
        store_plane(xp - 1, stresses(g, params(HP[xp - 1]), ALONG[0], flag("gx", 2 * side - 1)))

    for r in range(1, len(z_rounds)):
        told_z(r)
        tell_z(r + 1)
    told_x(1)
    tell_x(2)

    loads[4].wait()
    sums = [zero] * 8
    for x in range(8):
        xs = x + 1
        p_plane = PP[xs, block]
        slope = (
            PP[xs + 1, block] - PP[xs - 1, block],
            PP[xs, pl.ds(TOP + 1, 8)] - PP[xs, pl.ds(TOP - 1, 8)],
            across_z(p_plane, ends_of(near_halo, 48 + x)),
        )
        for i in range(3):
            loading = BF[i, x] - 0.5 * slope[i]
            cx, cy, cz = ALONG[0][i], ALONG[1][i], ALONG[2][i]
            out = []
            for f in range(6):
                change = SS[f, cx, xs + 1, block] - SS[f, cx, xs - 1, block]
                change = change + (SS[f, cy, xs, pl.ds(TOP + 1, 8)] - SS[f, cy, xs, pl.ds(TOP - 1, 8)])
                change = change + across_z(SS[f, cz, xs, block], ends_of(z_fields[f][cz], x))
                out.append(change if f == 1 else change + loading)
            chosen = out[5]
            for k in (2, 1, 0):
                chosen = jnp.where(picked == k, out[2 + k], chosen)
            CR[i, x] = chosen
            for k, a in enumerate(LENGTHS):
                sums[k] = sums[k] + out[2 + k] * out[2 + k]
                linear = out[0] + a * out[1]
                sums[4 + k] = sums[4 + k] + linear * linear

    stacked = zero
    for k in range(8):
        stacked = jnp.where(sub == k, jnp.sum(sums[k], axis=0, keepdims=True), stacked)
    totals = jnp.sum(stacked, axis=1, keepdims=True)
    row = jnp.sum(jnp.where(lane == sub, totals, 0.0), axis=0, keepdims=True)
    for stage, (axes, ref) in enumerate(((("gz",), RZ), (("gx", "gy"), RP))):
        offsets = [()]
        for a in axes:
            offsets = [o + (k,) for o in offsets for k in range(n[a])]
        hops = lambda o: sum(min(k, n[a] - k) for k, a in zip(o, axes))
        mine = 0
        for a in axes:
            mine = mine * n[a] + me[a]
        if len(axes) == 2:
            for r in range(2, len(x_rounds)):
                told_x(r)
                tell_x(r + 1)
        ref[mine] = row

        def share(rows, target):
            return pltpu.make_async_remote_copy(
                src_ref=rows, dst_ref=rows, send_sem=load_sem.at[stage], recv_sem=sum_sem.at[stage],
                device_id=target, device_id_type=MESH,
            )

        others = sorted((o for o in offsets if any(o)), key=lambda o: -hops(o))
        targets = [{a: lax.rem(me[a] + k, n[a]) for k, a in zip(o, axes)} for o in others]
        for target in targets:
            share(ref.at[mine], target).start()
        if stage == 0:
            sent()
        whole = share(ref.at[pl.ds(0, len(others))], targets[0])
        whole.wait_send()
        whole.wait_recv()
        rows = [ref[k] for k in range(len(offsets))]
        while len(rows) > 1:
            rows = [sum(rows[k:k + 2]) for k in range(0, len(rows), 2)]
        row = rows[0]
    cells = 3.0 * (8 * n["gx"]) * (8 * n["gy"]) * (128 * n["gz"])
    norms = jnp.sqrt(row / cells + 1e-6)
    norms_ref[pl.ds(0, 1)] = norms[:, 0:4]
    norms_ref[pl.ds(1, 1)] = roll(jnp.broadcast_to(norms, (8, 128)), -4, 1)[0:1, 0:4]


def write_out(*refs):
    copies = [pltpu.make_async_copy(refs[i], refs[3 + i], refs[6].at[i]) for i in range(3)]
    for copy in copies:
        copy.start()
    for copy in copies:
        copy.wait()


def solution(mesh):
    sizes = tuple(mesh.shape[a] for a in ("gx", "gy", "gz"))
    f32 = jnp.float32

    def body(*args):
        vector = jax.ShapeDtypeStruct((3, 8, 8, 128), f32)
        anywhere = pl.BlockSpec(memory_space=pl.ANY)
        inside = pl.BlockSpec(memory_space=pltpu.VMEM)
        args = [pltpu.with_memory_space_constraint(a, pltpu.HBM) for a in args[:8]] + [args[8]]
        outputs = (jax.ShapeDtypeStruct((2, 4), f32), vector, vector)
        found = pl.pallas_call(
            functools.partial(kernel, sizes),
            out_shape=outputs,
            in_specs=[pl.BlockSpec(memory_space=pltpu.HBM)] * 8 + [pl.BlockSpec(memory_space=pltpu.SMEM)],
            out_specs=(inside,) * 3,
            scratch_shapes=[
                pltpu.SMEM((4,), f32),
                pltpu.SMEM((4,), f32),
                pltpu.SMEM((4,), f32),
                pltpu.VMEM((6, 12, ROWS, 128), f32),
                pltpu.VMEM((10, ROWS, 128), f32),
                pltpu.VMEM((10, 8, 128), jnp.int32),
                pltpu.VMEM((3, 8, 8, 128), f32),
                pltpu.VMEM((2, 14, 8, 128), f32),
                pltpu.VMEM((2, 14, 8, 128), f32),
                pltpu.VMEM((3, 8, 128), f32),
                pltpu.VMEM((2, 2, 8, 128), f32),
                pltpu.VMEM((2, 2, 1, 8, 128), f32),
                pltpu.VMEM((2, 2, 2, 8, 128), f32),
                pltpu.VMEM((2, 2, 8, 128), f32),
                pltpu.VMEM((2, 2, 8, 128), f32),
                pltpu.VMEM((6, 6, 10, ROWS, 128), f32),
                pltpu.VMEM((3, 8, 8, 128), f32),
                pltpu.VMEM((sizes[2], 1, 128), f32),
                pltpu.VMEM((sizes[0] * sizes[1], 1, 128), f32),
                pltpu.SemaphoreType.DMA((4,)),
                pltpu.SemaphoreType.DMA((8,)),
                pltpu.SemaphoreType.DMA((8,)),
                pltpu.SemaphoreType.DMA((2,)),
                pltpu.SemaphoreType.REGULAR((2, 3)),
            ],
            compiler_params=pltpu.CompilerParams(
                collective_id=0, has_side_effects=True, vmem_limit_bytes=16 * 1024 * 1024
            ),
            name="line_search",
        )(*args)
        return pl.pallas_call(
            write_out,
            out_shape=outputs,
            in_specs=[inside] * 3,
            out_specs=(anywhere,) * 3,
            scratch_shapes=[pltpu.SemaphoreType.DMA((3,))],
            compiler_params=pltpu.CompilerParams(vmem_limit_bytes=4 * 1024 * 1024),
            name="write_out",
        )(*found)

    vector, scalar = P(None, "gx", "gy", "gz"), P("gx", "gy", "gz")
    return jax.shard_map(
        body,
        mesh=mesh,
        in_specs=(vector, vector, scalar, vector, scalar, P(), P(), P(), P()),
        out_specs=(P(), vector, vector),
        check_vma=False,
    )
```
